32 devices in a mesh: inp: 8 (over z, y), tm: 4 (over x, core).
Axes of the slice: x: 2, y: 2, z: 4, core: 2. Of those that a mesh axis runs over, the one named last changes fastest.
Arguments:
- voltages: bfloat16 [1024, 262144], P('inp', 'tm'), may hold values from -6 to 6
- pfb_coeff: float32 [16, 512], replicated, may hold values from -1.5 to 1.5
Outputs:
- visibilities: float32 [32, 2, 1024, 1024], P(('inp', 'tm'))
The draws below stay inside these ranges and needn't reach their ends.
All inputs are finite; a program needn't handle non-finite values.
Results may differ from the reference program's by a relative error of at most 0.0029.
Values may be sent and summed in bfloat16 or wider, within the bound.
A program may use at most 128 MiB of HBM per device.

```python
import math
import jax
import jax.numpy as jnp
from jax import lax

INPUTS = 1024
FFT_LEN = 512
TAPS = 16
CHAN = 32
SPECTRA = 512


def shard_levels(stream_key, extent, shards, low, high):
    def one(position, blocks):
        heights = jax.random.uniform(jax.random.fold_in(jax.random.fold_in(stream_key, 6), position), (blocks,), jnp.float32, low / len(shards), high / len(shards))
        return jnp.repeat(jnp.exp(heights), extent[position] // blocks).reshape((-1,) + (1,) * (len(extent) - position - 1))

    level = one(*shards[0])
    for cut in shards[1:]:
        level = level * one(*cut)
    return level


def bell_draw(key, dims, deviation, limit, shards=(), kind=jnp.bfloat16):
    result = jax.random.normal(key, dims, jnp.float32) * deviation
    if len(shards) > 0:
        result = shard_levels(key, dims, shards, -0.22, 0.18) * result
    return jnp.clip(result, min=-limit, max=limit).astype(kind)


def setup_inputs(seed: int = 0) -> dict:
    keys = jax.random.split(jax.random.key(seed), 3)
    voltages = bell_draw(keys[0], (INPUTS, SPECTRA * FFT_LEN), 1.0, 6.0, ((0, 8), (1, 4)))
    pfb_coeff = bell_draw(keys[1], (TAPS, FFT_LEN), TAPS ** -0.5, 1.5, (), jnp.float32)
    return dict(voltages=voltages, pfb_coeff=pfb_coeff)


def reference(voltages, pfb_coeff):
    input_block = math.gcd(INPUTS, 32)
    blocks = voltages.reshape(INPUTS // input_block, input_block, SPECTRA, FFT_LEN)

    def channelize(input_group):
        padded = jnp.concatenate([jnp.zeros((input_block, TAPS - 1, FFT_LEN), input_group.dtype), input_group], axis=1)
        filtered = jnp.zeros((input_block, SPECTRA, FFT_LEN), jnp.float32)
        for tap_index in range(TAPS):
            filtered = filtered + pfb_coeff[tap_index][None, None, :] * padded[:, tap_index:tap_index + SPECTRA, :].astype(jnp.float32)
        spectrum = jnp.fft.rfft(filtered, axis=-1)[:, :, :CHAN]
        norm_scale = 1.0 / math.sqrt(FFT_LEN)
        real_part = (jnp.real(spectrum) * norm_scale).astype(jnp.bfloat16)
        imag_part = (jnp.imag(spectrum) * norm_scale).astype(jnp.bfloat16)
        return jnp.stack([real_part, imag_part], axis=0)
    channelized = lax.map(channelize, blocks)
    channelized = jnp.transpose(channelized, (4, 1, 0, 2, 3)).reshape(CHAN, 2, INPUTS, SPECTRA)

    def gram_matrix(chan_data):
        real_part = chan_data[0].astype(jnp.float32)
        imag_part = chan_data[1].astype(jnp.float32)
        same_pol = jnp.dot(real_part, real_part.T, precision=lax.Precision.HIGHEST, preferred_element_type=jnp.float32)
        same_pol = same_pol + jnp.dot(imag_part, imag_part.T, precision=lax.Precision.HIGHEST, preferred_element_type=jnp.float32)
        cross_term = jnp.dot(imag_part, real_part.T, precision=lax.Precision.HIGHEST, preferred_element_type=jnp.float32)
        return jnp.stack([same_pol, cross_term - cross_term.T], axis=0) * (1.0 / SPECTRA)
    return lax.map(gram_matrix, channelized)
```

```python
import functools
import math

import jax
import jax.numpy as jnp
import numpy as np
from jax import lax
from jax.experimental import pallas as pl
from jax.experimental.pallas import tpu as pltpu
from jax.sharding import PartitionSpec as P

LANES = 128
ROWS = 16
GROUP = 8
CHUNK = 16
NT = (((1,), (1,)), ((), ()))


def dft_tables(channels, length):
    phase = np.arange(channels)[:, None] * np.arange(length)[None, :] % length
    angle = phase * (2.0 * math.pi / length)
    table = np.stack([np.cos(angle), -np.sin(angle)], axis=1) / math.sqrt(length)
    table = table.reshape(2 * channels, length).astype(np.float32)
    high = table.astype(jnp.bfloat16)
    low = (table - high.astype(np.float32)).astype(jnp.bfloat16)
    return np.concatenate([high, low], axis=0)


def channelize_kernel(
    n_inp, n_tm, volt, coef_in, table, out,
    slab, coef, high0, low0, high1, low1, stage, send,
    load_sem, tail_send, tail_recv, send_sem, recv_sem,
):
    in_rows = volt.shape[0]
    taps, length = coef_in.shape
    spec = volt.shape[1] // length
    lines = stage.shape[0] // CHUNK
    n_dev = n_inp * n_tm
    chunks = spec // CHUNK
    tail = (taps - 1) * length
    width = CHUNK * length
    a_tiles = in_rows // ROWS
    inp = lax.axis_index("inp")
    tm = lax.axis_index("tm")
    me = inp * n_tm + tm

    def load(q):
        return pltpu.make_async_copy(
            volt.at[:, pl.ds(pl.multiple_of(q * width, width), width)],
            slab.at[:, pl.ds(pl.multiple_of(tail + q * width, length), width)],
            load_sem.at[q],
        )

    load(0).start()
    load(1).start()

    barrier = pltpu.get_barrier_semaphore()

    def greet(d, _):
        other = lax.rem(me + d, n_dev)
        pl.semaphore_signal(
            barrier, inc=1, device_id=(other // n_tm, lax.rem(other, n_tm)),
            device_id_type=pl.DeviceIdType.MESH,
        )
        return _

    lax.fori_loop(1, n_dev, greet, 0)
    for j in range(taps):
        coef[j] = jnp.broadcast_to(coef_in[j : j + 1, :], (8, length))
    @pl.when(tm == 0)
    def _():
        def clear(e, _):
            slab[:, pl.ds(pl.multiple_of(e * length, length), length)] = jnp.zeros(
                (in_rows, length), slab.dtype
            )
            return _

        lax.fori_loop(0, taps - 1, clear, 0)

    f_high, f_low = (high0, high1), (low0, low1)

    def fir(first, tile, slot):
        row = pl.multiple_of(tile * ROWS, ROWS)
        for nt in range(length // LANES):
            lanes = pl.ds(nt * LANES, LANES)
            c = [coef[j, :, lanes] for j in range(taps)]
            low = [None] * GROUP
            high = [None] * GROUP
            for t in range(GROUP + taps - 1):
                col = pl.multiple_of((first + t) * length + nt * LANES, LANES)
                x = slab[pl.ds(row, ROWS), pl.ds(col, LANES)].astype(jnp.float32)
                x0, x1 = x[:8], x[8:]
                for i in range(max(0, t - taps + 1), min(GROUP - 1, t) + 1):
                    w = c[t - i]
                    if t == i:
                        low[i], high[i] = w * x0, w * x1
                    else:
                        low[i], high[i] = low[i] + w * x0, high[i] + w * x1
                i = t - taps + 1
                if i >= 0:
                    f = jnp.concatenate([low[i], high[i]], axis=0)
                    h = f.astype(jnp.bfloat16)
                    f_high[slot][i, pl.ds(row, ROWS), lanes] = h
                    f_low[slot][i, pl.ds(row, ROWS), lanes] = (
                        f - h.astype(jnp.float32)
                    ).astype(jnp.bfloat16)

    def dft(tile, slot):
        per = GROUP // a_tiles
        for u in range(per):
            i = tile * per + u
            r = lax.dot_general(table[...], f_high[slot][i], NT, preferred_element_type=jnp.float32)
            r2 = lax.dot_general(table[:lines], f_low[slot][i], NT, preferred_element_type=jnp.float32)
            stage[pl.ds(slot * GROUP + i, lines, stride=CHUNK), :] = r[:lines] + r[lines:] + r2

    def each(body):
        def step(tile, _):
            body(tile)
            return _

        lax.fori_loop(0, a_tiles, step, 0)

    def own(q):
        return pltpu.make_async_copy(send.at[q, me], place(out, q), recv_sem)

    def place(ref, q):
        first = pl.multiple_of(tm * spec + q * CHUNK, CHUNK)
        return ref.at[inp, :, pl.ds(first, CHUNK), :]

    def dispatch(q):
        def convert(d, _):
            rows = pl.ds(pl.multiple_of(d * 2 * CHUNK, 2 * CHUNK), 2 * CHUNK)
            send[q, d] = stage[rows, :].reshape(2, CHUNK, in_rows).astype(send.dtype)
            return _

        lax.fori_loop(0, n_dev, convert, 0)

        def post(d, _):
            other = lax.rem(me + d, n_dev)
            pltpu.make_async_remote_copy(
                src_ref=send.at[q, other], dst_ref=place(out, q),
                send_sem=send_sem, recv_sem=recv_sem,
                device_id=(other // n_tm, lax.rem(other, n_tm)),
                device_id_type=pl.DeviceIdType.MESH,
            ).start()
            return _

        lax.fori_loop(1, n_dev, post, 0)
        own(q).start()

    def chunk_of(k):
        return lax.rem(k + 1, chunks)

    load(0).wait()
    load(1).wait()
    for q in range(2, chunks):
        load(q).start()
    each(lambda tile: fir(chunk_of(0) * CHUNK, tile, 0))
    pl.semaphore_wait(barrier, n_dev - 1)

    history = pltpu.make_async_remote_copy(
        src_ref=volt.at[:, pl.ds(spec * length - tail, tail)],
        dst_ref=slab.at[:, pl.ds(0, tail)],
        send_sem=tail_send, recv_sem=tail_recv,
        device_id=(inp, lax.rem(tm + 1, n_tm)),
        device_id_type=pl.DeviceIdType.MESH,
    )

    @pl.when(tm < n_tm - 1)
    def _():
        history.start()

    def turn(k, carry):
        q = chunk_of(k)
        later = chunk_of(k + 1)

        def second(tile):
            dft(tile, 0)
            fir(q * CHUNK + GROUP, tile, 1)

        each(second)

        @pl.when(later > 0)
        def _():
            load(later).wait()

        @pl.when((later == 0) & (tm > 0))
        def _():
            history.wait_recv()

        def first(tile):
            dft(tile, 1)
            fir(later * CHUNK, tile, 0)

        each(first)
        dispatch(q)
        return carry

    lax.fori_loop(0, chunks - 1, turn, 0)

    def final(tile):
        dft(tile, 0)
        fir(GROUP, tile, 1)

    each(final)
    each(lambda tile: dft(tile, 1))
    dispatch(0)

    @pl.when(tm < n_tm - 1)
    def _():
        history.wait_send()

    sent = send.at[:, pl.ds(0, n_dev - 1)]
    pltpu.make_async_copy(sent, sent, send_sem).wait()
    pltpu.make_async_copy(out, out, recv_sem).wait()


def correlate_kernel(z_ref, o_ref, wide, turned, crossed):
    groups, _, spectra, in_rows = z_ref.shape
    block = o_ref.shape[2]

    @pl.when(pl.program_id(0) == 0)
    def _():
        for g in range(groups):
            cols = slice(g * in_rows, (g + 1) * in_rows)
            for p in range(2):
                part = z_ref[g, p]
                wide[p * spectra : (p + 1) * spectra, cols] = part
                flip = part.T
                turned[cols, p * spectra : (p + 1) * spectra] = flip
                crossed[cols, (1 - p) * spectra : (2 - p) * spectra] = flip if p else -flip

    rows = pl.ds(pl.multiple_of(pl.program_id(0) * block, block), block)
    scale = 1.0 / spectra
    o_ref[0, 0] = jnp.dot(turned[rows, :], wide[...], preferred_element_type=jnp.float32) * scale
    o_ref[0, 1] = jnp.dot(crossed[rows, :], wide[...], preferred_element_type=jnp.float32) * scale


def narrow_device(voltages, pfb_coeff):
    n_inp = lax.axis_size("inp")
    n_tm = lax.axis_size("tm")
    channels = n_inp * n_tm
    in_rows = voltages.shape[0]
    taps, length = pfb_coeff.shape
    spec = voltages.shape[1] // length
    lines = 2 * channels
    table = jnp.asarray(dft_tables(channels, length))
    vmem = pl.BlockSpec(memory_space=pltpu.VMEM)
    hbm = pl.BlockSpec(memory_space=pl.ANY)
    bf16 = jnp.bfloat16
    received = pl.pallas_call(
        functools.partial(channelize_kernel, n_inp, n_tm),
        out_shape=jax.ShapeDtypeStruct((n_inp, 2, n_tm * spec, in_rows), bf16),
        in_specs=[hbm, vmem, vmem],
        out_specs=hbm,
        scratch_shapes=[
            pltpu.VMEM((in_rows, (spec + taps - 1) * length), bf16),
            pltpu.VMEM((taps, 8, length), jnp.float32),
            pltpu.VMEM((GROUP, in_rows, length), bf16),
            pltpu.VMEM((GROUP, in_rows, length), bf16),
            pltpu.VMEM((GROUP, in_rows, length), bf16),
            pltpu.VMEM((GROUP, in_rows, length), bf16),
            pltpu.VMEM((lines * CHUNK, in_rows), jnp.float32),
            pltpu.VMEM((spec // CHUNK, channels, 2, CHUNK, in_rows), bf16),
            pltpu.SemaphoreType.DMA((spec // CHUNK,)),
            pltpu.SemaphoreType.DMA,
            pltpu.SemaphoreType.DMA,
            pltpu.SemaphoreType.DMA,
            pltpu.SemaphoreType.DMA,
        ],
        compiler_params=pltpu.CompilerParams(
            collective_id=0, has_side_effects=True, vmem_limit_bytes=60 * 1024 * 1024
        ),
        name="channelize",
    )(voltages, pfb_coeff, table)
    inputs = n_inp * in_rows
    spectra = n_tm * spec
    block = min(256, inputs)
    return pl.pallas_call(
        correlate_kernel,
        grid=(inputs // block,),
        out_shape=jax.ShapeDtypeStruct((1, 2, inputs, inputs), jnp.float32),
        in_specs=[pl.BlockSpec(received.shape, lambda i: (0, 0, 0, 0))],
        out_specs=pl.BlockSpec((1, 2, block, inputs), lambda i: (0, 0, i, 0)),
        scratch_shapes=[
            pltpu.VMEM((2 * spectra, inputs), bf16),
            pltpu.VMEM((inputs, 2 * spectra), bf16),
            pltpu.VMEM((inputs, 2 * spectra), bf16),
        ],
        compiler_params=pltpu.CompilerParams(vmem_limit_bytes=60 * 1024 * 1024),
        name="correlate",
    )(received)


STEP = 8
PART = 4


def split_table(channels, length):
    phase = np.arange(channels)[:, None] * np.arange(length)[None, :] % length
    angle = phase * (2.0 * math.pi / length)
    table = np.stack([np.cos(angle), -np.sin(angle)], axis=1) / math.sqrt(length)
    return table.reshape(2 * channels, length).astype(np.float32)


def stream_kernel(
    n_inp, n_tm, volt, coef_in, table, out,
    slab, taps_table, prod, acc, head, tail_out, tail_in, stage, send,
    load_sem, tail_send, tail_recv, send_sem, recv_sem,
):
    in_rows = volt.shape[0]
    taps, length = coef_in.shape
    steps = volt.shape[1] // (length * STEP)
    lines = table.shape[0]
    n_dev = n_inp * n_tm
    width = STEP * length
    inp = lax.axis_index("inp")
    tm = lax.axis_index("tm")
    me = inp * n_tm + tm
    heads = (taps + STEP - 1) // STEP
    turn = steps - heads

    def load(i):
        cols = pl.ds(pl.multiple_of(i * width, width), width)
        return pltpu.make_async_copy(volt.at[:, cols], slab.at[:, cols], load_sem.at[i])

    def step_of(t):
        return lax.rem(t + heads, steps)

    for t in range(steps):
        load((t + heads) % steps).start()

    barrier = pltpu.get_barrier_semaphore()

    def greet(d, _):
        other = lax.rem(me + d, n_dev)
        pl.semaphore_signal(
            barrier, inc=1, device_id=(other // n_tm, lax.rem(other, n_tm)),
            device_id_type=pl.DeviceIdType.MESH,
        )
        return _

    lax.fori_loop(1, n_dev, greet, 0)

    def build(j, _):
        full = table[...] * coef_in[pl.ds(j, 1), :]
        high = full.astype(jnp.bfloat16)
        rows = pl.ds(pl.multiple_of(j * lines, lines), lines)
        taps_table[rows, :length] = high
        taps_table[rows, length:] = (full - high.astype(jnp.float32)).astype(jnp.bfloat16)
        return _

    lax.fori_loop(0, taps, build, 0)
    acc[...] = jnp.zeros(acc.shape, acc.dtype)

    half = n_inp // 2
    side = inp // half
    fars = [(1 - side) * half + lax.rem(inp + d, half) for d in range(half)]
    nears = [side * half + lax.rem(inp + d, half) for d in range(half)]
    cores = [lax.rem(tm + d, n_tm) for d in range(n_tm)]

    def place(i):
        return out.at[inp, tm * steps + i]

    def dispatch(i):
        send[i] = stage[...].reshape(n_dev, 2 * STEP, in_rows).astype(send.dtype)

        def post(inp2, tm2):
            pltpu.make_async_remote_copy(
                src_ref=send.at[i, inp2 * n_tm + tm2], dst_ref=place(i),
                send_sem=send_sem, recv_sem=recv_sem,
                device_id=(inp2, tm2), device_id_type=pl.DeviceIdType.MESH,
            ).start()

        for row in fars:
            for core in cores:
                post(row, core)
        for d, row in enumerate(nears):
            for core in cores[d == 0 :]:
                post(row, core)
        pltpu.make_async_copy(send.at[i, me], place(i), recv_sem).start()

    def advance(i):
        first = i * width
        for h in range(STEP // PART):
            x = jnp.concatenate(
                [
                    slab[:, pl.ds(pl.multiple_of(first + (h * PART + u) * length, length), length)]
                    for u in range(PART)
                ],
                axis=0,
            )
            x = jnp.concatenate([x, x], axis=1)
            prod[h] = lax.dot_general(taps_table[...], x, NT, preferred_element_type=jnp.float32)
            for k in range(taps + PART - 1):
                total = acc[k] if k < taps - 1 else None
                for u in range(PART):
                    j = u + taps - 1 - k
                    if 0 <= j < taps:
                        term = prod[h, j * lines : (j + 1) * lines, u * in_rows : (u + 1) * in_rows]
                        total = term if total is None else total + term
                if k < PART:
                    stage[pl.ds(h * PART + k, lines, stride=STEP), :] = total
                else:
                    acc[k - PART] = total

    def finish(w, source):
        for q in range(heads):
            for k in range(STEP):
                rows = pl.ds(k, lines, stride=STEP)
                total = head[q + (0 if w else heads), rows, :]
                s = q * STEP + k
                stage[rows, :] = total + source[s] if s < taps - 1 else total
            dispatch(q + (0 if w else heads))

    history = pltpu.make_async_remote_copy(
        src_ref=tail_out, dst_ref=tail_in, send_sem=tail_send, recv_sem=tail_recv,
        device_id=(inp, lax.rem(tm + 1, n_tm)), device_id_type=pl.DeviceIdType.MESH,
    )

    def work(t, carry):
        i = step_of(t)
        load(i).wait()

        @pl.when(t == heads)
        def _():
            pl.semaphore_wait(barrier, n_dev - 1)

        @pl.when(t == turn)
        def _():
            tail_out[...] = acc[...]
            acc[...] = jnp.zeros(acc.shape, acc.dtype)

            @pl.when(tm < n_tm - 1)
            def _():
                history.start()

        advance(i)
        @pl.when((t < heads) | (t >= turn))
        def _():
            head[i] = stage[...]

        @pl.when((t >= heads) & (t < turn))
        def _():
            dispatch(i)

        return carry

    lax.fori_loop(0, steps, work, 0)
    finish(0, acc)

    @pl.when(tm > 0)
    def _():
        history.wait_recv()

    @pl.when(tm == 0)
    def _():
        tail_in[...] = jnp.zeros(tail_in.shape, tail_in.dtype)

    finish(1, tail_in)

    @pl.when(tm < n_tm - 1)
    def _():
        history.wait_send()

    sent = send.at[:, pl.ds(0, n_dev - 1)]
    pltpu.make_async_copy(sent, sent, send_sem).wait()
    pltpu.make_async_copy(out, out, recv_sem).wait()


def gram_kernel(z_ref, o_ref, wide, cross, turned):
    groups, chunks, pair, in_rows = z_ref.shape
    depth = chunks * pair
    spectra = depth // 2
    block = o_ref.shape[2]

    @pl.when(pl.program_id(0) == 0)
    def _():
        for g in range(groups):
            cols = slice(g * in_rows, (g + 1) * in_rows)
            part = z_ref[g]
            flat = part.reshape(depth, in_rows)
            wide[:, cols] = flat
            turned[cols, :] = flat.T
            full = part.astype(jnp.float32)
            swap = jnp.concatenate([-full[:, pair // 2 :], full[:, : pair // 2]], axis=1)
            cross[:, cols] = swap.astype(part.dtype).reshape(depth, in_rows)

    rows = pl.ds(pl.multiple_of(pl.program_id(0) * block, block), block)
    scale = 1.0 / spectra
    left = turned[rows, :]
    o_ref[0, 0] = jnp.dot(left, wide[...], preferred_element_type=jnp.float32) * scale
    o_ref[0, 1] = jnp.dot(left, cross[...], preferred_element_type=jnp.float32) * scale


def stream_device(voltages, pfb_coeff):
    n_inp = lax.axis_size("inp")
    n_tm = lax.axis_size("tm")
    channels = n_inp * n_tm
    in_rows = voltages.shape[0]
    taps, length = pfb_coeff.shape
    steps = voltages.shape[1] // (length * STEP)
    lines = 2 * channels
    heads = (taps + STEP - 1) // STEP
    table = jnp.asarray(split_table(channels, length))
    vmem = pl.BlockSpec(memory_space=pltpu.VMEM)
    hbm = pl.BlockSpec(memory_space=pl.ANY)
    bf16, f32 = jnp.bfloat16, jnp.float32
    carry = (taps - 1, lines, in_rows)
    received = pl.pallas_call(
        functools.partial(stream_kernel, n_inp, n_tm),
        out_shape=jax.ShapeDtypeStruct((n_inp, n_tm * steps, 2 * STEP, in_rows), bf16),
        in_specs=[hbm, vmem, vmem],
        out_specs=hbm,
        scratch_shapes=[
            pltpu.VMEM(voltages.shape, bf16),
            pltpu.VMEM((taps * lines, 2 * length), bf16),
            pltpu.VMEM((STEP // PART, taps * lines, PART * in_rows), f32),
            pltpu.VMEM(carry, f32),
            pltpu.VMEM((2 * heads, lines * STEP, in_rows), f32),
            pltpu.VMEM(carry, f32),
            pltpu.VMEM(carry, f32),
            pltpu.VMEM((lines * STEP, in_rows), f32),
            pltpu.VMEM((steps, channels, 2 * STEP, in_rows), bf16),
            pltpu.SemaphoreType.DMA((steps,)),
            pltpu.SemaphoreType.DMA,
            pltpu.SemaphoreType.DMA,
            pltpu.SemaphoreType.DMA,
            pltpu.SemaphoreType.DMA,
        ],
        compiler_params=pltpu.CompilerParams(
            collective_id=0, has_side_effects=True, vmem_limit_bytes=60 * 1024 * 1024
        ),
        name="stream",
    )(voltages, pfb_coeff, table)
    inputs = n_inp * in_rows
    depth = n_tm * steps * 2 * STEP
    block = min(256, inputs)
    return pl.pallas_call(
        gram_kernel,
        grid=(inputs // block,),
        out_shape=jax.ShapeDtypeStruct((1, 2, inputs, inputs), f32),
        in_specs=[pl.BlockSpec(received.shape, lambda i: (0, 0, 0, 0))],
        out_specs=pl.BlockSpec((1, 2, block, inputs), lambda i: (0, 0, i, 0)),
        scratch_shapes=[
            pltpu.VMEM((depth, inputs), bf16),
            pltpu.VMEM((depth, inputs), bf16),
            pltpu.VMEM((inputs, depth), bf16),
        ],
        compiler_params=pltpu.CompilerParams(vmem_limit_bytes=60 * 1024 * 1024),
        name="gram",
    )(received)


def per_device(voltages, pfb_coeff):
    if voltages.shape[0] % LANES == 0:
        return stream_device(voltages, pfb_coeff)
    return narrow_device(voltages, pfb_coeff)


def solution(mesh):
    return jax.shard_map(
        per_device,
        mesh=mesh,
        in_specs=(P("inp", "tm"), P()),
        out_specs=P(("inp", "tm"), None, None, None),
        check_vma=False,
    )
```

```python
import functools
import math

import jax
import jax.numpy as jnp
import numpy as np
from jax import lax
from jax.experimental import pallas as pl
from jax.experimental.pallas import tpu as pltpu
from jax.sharding import PartitionSpec as P

LANES = 128
ROWS = 16
GROUP = 8
CHUNK = 16
NT = (((1,), (1,)), ((), ()))


def dft_tables(channels, length):
    phase = np.arange(channels)[:, None] * np.arange(length)[None, :] % length
    angle = phase * (2.0 * math.pi / length)
    table = np.stack([np.cos(angle), -np.sin(angle)], axis=1) / math.sqrt(length)
    table = table.reshape(2 * channels, length).astype(np.float32)
    high = table.astype(jnp.bfloat16)
    low = (table - high.astype(np.float32)).astype(jnp.bfloat16)
    return np.concatenate([high, low], axis=0)


def channelize_kernel(
    n_inp, n_tm, volt, coef_in, table, out,
    slab, coef, high0, low0, high1, low1, stage, send,
    load_sem, tail_send, tail_recv, send_sem, recv_sem,
):
    in_rows = volt.shape[0]
    taps, length = coef_in.shape
    spec = volt.shape[1] // length
    lines = stage.shape[0] // CHUNK
    n_dev = n_inp * n_tm
    chunks = spec // CHUNK
    tail = (taps - 1) * length
    width = CHUNK * length
    a_tiles = in_rows // ROWS
    inp = lax.axis_index("inp")
    tm = lax.axis_index("tm")
    me = inp * n_tm + tm

    def load(q):
        return pltpu.make_async_copy(
            volt.at[:, pl.ds(pl.multiple_of(q * width, width), width)],
            slab.at[:, pl.ds(pl.multiple_of(tail + q * width, length), width)],
            load_sem.at[q],
        )

    load(0).start()
    load(1).start()

    barrier = pltpu.get_barrier_semaphore()

    def greet(d, _):
        other = lax.rem(me + d, n_dev)
        pl.semaphore_signal(
            barrier, inc=1, device_id=(other // n_tm, lax.rem(other, n_tm)),
            device_id_type=pl.DeviceIdType.MESH,
        )
        return _

    lax.fori_loop(1, n_dev, greet, 0)
    for j in range(taps):
        coef[j] = jnp.broadcast_to(coef_in[j : j + 1, :], (8, length))
    @pl.when(tm == 0)
    def _():
        def clear(e, _):
            slab[:, pl.ds(pl.multiple_of(e * length, length), length)] = jnp.zeros(
                (in_rows, length), slab.dtype
            )
            return _

        lax.fori_loop(0, taps - 1, clear, 0)

    f_high, f_low = (high0, high1), (low0, low1)

    def fir(first, tile, slot):
        row = pl.multiple_of(tile * ROWS, ROWS)
        for nt in range(length // LANES):
            lanes = pl.ds(nt * LANES, LANES)
            c = [coef[j, :, lanes] for j in range(taps)]
            low = [None] * GROUP
            high = [None] * GROUP
            for t in range(GROUP + taps - 1):
                col = pl.multiple_of((first + t) * length + nt * LANES, LANES)
                x = slab[pl.ds(row, ROWS), pl.ds(col, LANES)].astype(jnp.float32)
                x0, x1 = x[:8], x[8:]
                for i in range(max(0, t - taps + 1), min(GROUP - 1, t) + 1):
                    w = c[t - i]
                    if t == i:
                        low[i], high[i] = w * x0, w * x1
                    else:
                        low[i], high[i] = low[i] + w * x0, high[i] + w * x1
                i = t - taps + 1
                if i >= 0:
                    f = jnp.concatenate([low[i], high[i]], axis=0)
                    h = f.astype(jnp.bfloat16)
                    f_high[slot][i, pl.ds(row, ROWS), lanes] = h
                    f_low[slot][i, pl.ds(row, ROWS), lanes] = (
                        f - h.astype(jnp.float32)
                    ).astype(jnp.bfloat16)

    def dft(tile, slot):
        per = GROUP // a_tiles
        for u in range(per):
            i = tile * per + u
            r = lax.dot_general(table[...], f_high[slot][i], NT, preferred_element_type=jnp.float32)
            r2 = lax.dot_general(table[:lines], f_low[slot][i], NT, preferred_element_type=jnp.float32)
            stage[pl.ds(slot * GROUP + i, lines, stride=CHUNK), :] = r[:lines] + r[lines:] + r2

    def each(body):
        def step(tile, _):
            body(tile)
            return _

        lax.fori_loop(0, a_tiles, step, 0)

    def own(q):
        return pltpu.make_async_copy(send.at[q, me], place(out, q), recv_sem)

    def place(ref, q):
        first = pl.multiple_of(tm * spec + q * CHUNK, CHUNK)
        return ref.at[inp, :, pl.ds(first, CHUNK), :]

    def dispatch(q):
        def convert(d, _):
            rows = pl.ds(pl.multiple_of(d * 2 * CHUNK, 2 * CHUNK), 2 * CHUNK)
            send[q, d] = stage[rows, :].reshape(2, CHUNK, in_rows).astype(send.dtype)
            return _

        lax.fori_loop(0, n_dev, convert, 0)

        def post(d, _):
            other = lax.rem(me + d, n_dev)
            pltpu.make_async_remote_copy(
                src_ref=send.at[q, other], dst_ref=place(out, q),
                send_sem=send_sem, recv_sem=recv_sem,
                device_id=(other // n_tm, lax.rem(other, n_tm)),
                device_id_type=pl.DeviceIdType.MESH,
            ).start()
            return _

        lax.fori_loop(1, n_dev, post, 0)
        own(q).start()

    def chunk_of(k):
        return lax.rem(k + 1, chunks)

    load(0).wait()
    load(1).wait()
    for q in range(2, chunks):
        load(q).start()
    each(lambda tile: fir(chunk_of(0) * CHUNK, tile, 0))
    pl.semaphore_wait(barrier, n_dev - 1)

    history = pltpu.make_async_remote_copy(
        src_ref=volt.at[:, pl.ds(spec * length - tail, tail)],
        dst_ref=slab.at[:, pl.ds(0, tail)],
        send_sem=tail_send, recv_sem=tail_recv,
        device_id=(inp, lax.rem(tm + 1, n_tm)),
        device_id_type=pl.DeviceIdType.MESH,
    )

    @pl.when(tm < n_tm - 1)
    def _():
        history.start()

    def turn(k, carry):
        q = chunk_of(k)
        later = chunk_of(k + 1)

        def second(tile):
            dft(tile, 0)
            fir(q * CHUNK + GROUP, tile, 1)

        each(second)

        @pl.when(later > 0)
        def _():
            load(later).wait()

        @pl.when((later == 0) & (tm > 0))
        def _():
            history.wait_recv()

        def first(tile):
            dft(tile, 1)
            fir(later * CHUNK, tile, 0)

        each(first)
        dispatch(q)
        return carry

    lax.fori_loop(0, chunks - 1, turn, 0)

    def final(tile):
        dft(tile, 0)
        fir(GROUP, tile, 1)

    each(final)
    each(lambda tile: dft(tile, 1))
    dispatch(0)

    @pl.when(tm < n_tm - 1)
    def _():
        history.wait_send()

    sent = send.at[:, pl.ds(0, n_dev - 1)]
    pltpu.make_async_copy(sent, sent, send_sem).wait()
    pltpu.make_async_copy(out, out, recv_sem).wait()


def correlate_kernel(z_ref, o_ref, wide, turned, crossed):
    groups, _, spectra, in_rows = z_ref.shape
    block = o_ref.shape[2]

    @pl.when(pl.program_id(0) == 0)
    def _():
        for g in range(groups):
            cols = slice(g * in_rows, (g + 1) * in_rows)
            for p in range(2):
                part = z_ref[g, p]
                wide[p * spectra : (p + 1) * spectra, cols] = part
                flip = part.T
                turned[cols, p * spectra : (p + 1) * spectra] = flip
                crossed[cols, (1 - p) * spectra : (2 - p) * spectra] = flip if p else -flip

    rows = pl.ds(pl.multiple_of(pl.program_id(0) * block, block), block)
    scale = 1.0 / spectra
    o_ref[0, 0] = jnp.dot(turned[rows, :], wide[...], preferred_element_type=jnp.float32) * scale
    o_ref[0, 1] = jnp.dot(crossed[rows, :], wide[...], preferred_element_type=jnp.float32) * scale


def narrow_device(voltages, pfb_coeff):
    n_inp = lax.axis_size("inp")
    n_tm = lax.axis_size("tm")
    channels = n_inp * n_tm
    in_rows = voltages.shape[0]
    taps, length = pfb_coeff.shape
    spec = voltages.shape[1] // length
    lines = 2 * channels
    table = jnp.asarray(dft_tables(channels, length))
    vmem = pl.BlockSpec(memory_space=pltpu.VMEM)
    hbm = pl.BlockSpec(memory_space=pl.ANY)
    bf16 = jnp.bfloat16
    received = pl.pallas_call(
        functools.partial(channelize_kernel, n_inp, n_tm),
        out_shape=jax.ShapeDtypeStruct((n_inp, 2, n_tm * spec, in_rows), bf16),
        in_specs=[hbm, vmem, vmem],
        out_specs=hbm,
        scratch_shapes=[
            pltpu.VMEM((in_rows, (spec + taps - 1) * length), bf16),
            pltpu.VMEM((taps, 8, length), jnp.float32),
            pltpu.VMEM((GROUP, in_rows, length), bf16),
            pltpu.VMEM((GROUP, in_rows, length), bf16),
            pltpu.VMEM((GROUP, in_rows, length), bf16),
            pltpu.VMEM((GROUP, in_rows, length), bf16),
            pltpu.VMEM((lines * CHUNK, in_rows), jnp.float32),
            pltpu.VMEM((spec // CHUNK, channels, 2, CHUNK, in_rows), bf16),
            pltpu.SemaphoreType.DMA((spec // CHUNK,)),
            pltpu.SemaphoreType.DMA,
            pltpu.SemaphoreType.DMA,
            pltpu.SemaphoreType.DMA,
            pltpu.SemaphoreType.DMA,
        ],
        compiler_params=pltpu.CompilerParams(
            collective_id=0, has_side_effects=True, vmem_limit_bytes=60 * 1024 * 1024
        ),
        name="channelize",
    )(voltages, pfb_coeff, table)
    inputs = n_inp * in_rows
    spectra = n_tm * spec
    block = min(256, inputs)
    return pl.pallas_call(
        correlate_kernel,
        grid=(inputs // block,),
        out_shape=jax.ShapeDtypeStruct((1, 2, inputs, inputs), jnp.float32),
        in_specs=[pl.BlockSpec(received.shape, lambda i: (0, 0, 0, 0))],
        out_specs=pl.BlockSpec((1, 2, block, inputs), lambda i: (0, 0, i, 0)),
        scratch_shapes=[
            pltpu.VMEM((2 * spectra, inputs), bf16),
            pltpu.VMEM((inputs, 2 * spectra), bf16),
            pltpu.VMEM((inputs, 2 * spectra), bf16),
        ],
        compiler_params=pltpu.CompilerParams(vmem_limit_bytes=60 * 1024 * 1024),
        name="correlate",
    )(received)


STEP = 8
PART = 4
SPAN = 4
BLOCK = 256
AHEAD = 3
TINY = jnp.float8_e5m2
LIFT = 2.0**12
GAIN = 2.0**38


def split_table(channels, length):
    phase = np.arange(channels)[:, None] * np.arange(length)[None, :] % length
    angle = phase * (2.0 * math.pi / length)
    table = np.stack([np.cos(angle), -np.sin(angle)], axis=1) / math.sqrt(length)
    return table.reshape(2 * channels, length).astype(np.float32)


def stream_kernel(
    n_inp, n_tm, volt, coef_from, table_from, part, last,
    coef_in, table, slab, taps_table, low_table, thin, acc, head, tail_out, tail_in, stage, send,
    landed, wide, cross, turned, small_sem, load_sem, tail_send, tail_recv, send_sem, recv_sem,
):
    in_rows = volt.shape[0]
    taps, length = coef_from.shape
    steps = volt.shape[1] // (length * STEP)
    lines = table_from.shape[0]
    n_dev = n_inp * n_tm
    width = STEP * length
    inp = lax.axis_index("inp")
    tm = lax.axis_index("tm")
    me = inp * n_tm + tm
    heads = (taps + STEP - 1) // STEP
    turn = steps - heads

    def load(i):
        cols = pl.ds(pl.multiple_of(i * width, width), width)
        return pltpu.make_async_copy(volt.at[:, cols], slab.at[:, cols], load_sem.at[i])

    def step_of(t):
        return lax.rem(t + heads, steps)

    small = [
        pltpu.make_async_copy(source, target, small_sem.at[n])
        for n, (source, target) in enumerate(((coef_from, coef_in), (table_from, table)))
    ]
    for copy in small:
        copy.start()
    for t in range(AHEAD):
        load((t + heads) % steps).start()

    barrier = pltpu.get_barrier_semaphore()

    def greet(d, _):
        other = lax.rem(me + d, n_dev)
        pl.semaphore_signal(
            barrier, inc=1, device_id=(other // n_tm, lax.rem(other, n_tm)),
            device_id_type=pl.DeviceIdType.MESH,
        )
        return _

    lax.fori_loop(1, n_dev, greet, 0)
    for copy in small:
        copy.wait()

    def build(j, _):
        full = table[...] * coef_in[pl.ds(j, 1), :] * GAIN
        high = full.astype(jnp.bfloat16)
        rows = pl.ds(pl.multiple_of(j * lines, lines), lines)
        taps_table[rows, :] = high
        low_table[rows, :] = ((full - high.astype(jnp.float32)) / LIFT).astype(TINY)
        return _

    lax.fori_loop(0, taps, build, 0)
    acc[...] = jnp.zeros(acc.shape, acc.dtype)

    half = n_inp // 2
    side = inp // half
    fars = [(1 - side) * half + lax.rem(inp + d, half) for d in range(half)]
    nears = [side * half + lax.rem(inp + d, half) for d in range(half)]
    cores = [lax.rem(tm + d, n_tm) for d in range(n_tm)]

    def slot(i):
        return me * SPAN + lax.rem(i, SPAN)

    def bank(group):
        return last if isinstance(group, int) and group == 0 else landed.at[group - 1]

    def dispatch(i):
        send[i] = (stage[...] * (1.0 / GAIN)).reshape(n_dev, 2 * STEP, in_rows).astype(send.dtype)
        group = i // SPAN
        target = bank(group)

        def post(inp2, tm2):
            pltpu.make_async_remote_copy(
                src_ref=send.at[i, inp2 * n_tm + tm2], dst_ref=target.at[slot(i)],
                send_sem=send_sem, recv_sem=recv_sem.at[group],
                device_id=(inp2, tm2), device_id_type=pl.DeviceIdType.MESH,
            ).start()

        for row in fars:
            for core in cores:
                post(row, core)
        for d, row in enumerate(nears):
            for core in cores[d == 0 :]:
                post(row, core)
        target[slot(i)] = send[i, me]

    def advance(i):
        first = i * width
        for h in range(STEP // PART):
            x = jnp.concatenate(
                [
                    slab[:, pl.ds(pl.multiple_of(first + (h * PART + u) * length, length), length)]
                    for u in range(PART)
                ],
                axis=0,
            )
            thin[h] = (x.astype(jnp.float32) * LIFT).astype(TINY)
            high = lax.dot_general(taps_table[...], x, NT, preferred_element_type=jnp.float32)
            low = lax.dot_general(low_table[...], thin[h], NT, preferred_element_type=jnp.float32)
            for k in range(taps + PART - 1):
                total = acc[k] if k < taps - 1 else None
                for u in range(PART):
                    j = u + taps - 1 - k
                    if 0 <= j < taps:
                        spot = (slice(j * lines, (j + 1) * lines), slice(u * in_rows, (u + 1) * in_rows))
                        term = high[spot] + low[spot]
                        total = term if total is None else total + term
                if k < PART:
                    stage[pl.ds(h * PART + k, lines, stride=STEP), :] = total
                else:
                    acc[k - PART] = total

    def finish(w, source):
        for q in range(heads):
            for k in range(STEP):
                rows = pl.ds(k, lines, stride=STEP)
                total = head[q + (0 if w else heads), rows, :]
                s = q * STEP + k
                stage[rows, :] = total + source[s] if s < taps - 1 else total
            dispatch(q + (0 if w else heads))

    history = pltpu.make_async_remote_copy(
        src_ref=tail_out, dst_ref=tail_in, send_sem=tail_send, recv_sem=tail_recv,
        device_id=(inp, lax.rem(tm + 1, n_tm)), device_id_type=pl.DeviceIdType.MESH,
    )

    def work(t, carry):
        i = step_of(t)
        load(i).wait()

        @pl.when(t < steps - AHEAD)
        def _():
            load(step_of(t + AHEAD)).start()

        @pl.when(t == heads)
        def _():
            pl.semaphore_wait(barrier, n_dev - 1)

        @pl.when(t == turn)
        def _():
            tail_out[...] = acc[...]
            acc[...] = jnp.zeros(acc.shape, acc.dtype)

            @pl.when(tm < n_tm - 1)
            def _():
                history.start()

        advance(i)
        @pl.when((t < heads) | (t >= turn))
        def _():
            head[i] = stage[...]

        @pl.when((t >= heads) & (t < turn))
        def _():
            dispatch(i)

        return carry

    lax.fori_loop(0, steps, work, 0)
    finish(0, acc)

    def arrive(group):
        came = bank(group).at[pl.ds(0, (n_dev - 1) * SPAN)]
        pltpu.make_async_copy(came, came, recv_sem.at[group]).wait()

    def fold(group):
        arrive(group)
        pack(bank(group), wide, cross, turned)

        def block(b, carry):
            rows = pl.ds(pl.multiple_of(b * BLOCK, BLOCK), BLOCK)
            left = turned[rows, :]
            for p, right in enumerate((wide, cross)):
                term = jnp.dot(left, right[...], preferred_element_type=jnp.float32)
                part[p, rows, :] = term if group == 1 else part[p, rows, :] + term
            return carry

        lax.fori_loop(0, part.shape[1] // BLOCK, block, 0)

    for group in range(1, steps // SPAN - 1):
        fold(group)

    @pl.when(tm > 0)
    def _():
        history.wait_recv()

    @pl.when(tm == 0)
    def _():
        tail_in[...] = jnp.zeros(tail_in.shape, tail_in.dtype)

    finish(1, tail_in)
    fold(steps // SPAN - 1)

    @pl.when(tm < n_tm - 1)
    def _():
        history.wait_send()

    sent = send.at[:, pl.ds(0, n_dev - 1)]
    pltpu.make_async_copy(sent, sent, send_sem).wait()
    arrive(0)


def pack(source, wide, cross, turned):
    depth, inputs = wide.shape
    tiles, pair, in_rows = source.shape
    span = depth // pair
    for g in range(inputs // in_rows):
        cols = slice(g * in_rows, (g + 1) * in_rows)
        piece = source[g * span : (g + 1) * span]
        flat = piece.reshape(depth, in_rows)
        wide[:, cols] = flat
        turned[cols, :] = flat.T
        full = piece.astype(jnp.float32)
        swap = jnp.concatenate([-full[:, pair // 2 :], full[:, : pair // 2]], axis=1)
        cross[:, cols] = swap.astype(piece.dtype).reshape(depth, in_rows)


def close_kernel(spectra, part, last, out, wide, cross, turned, done, sem):
    pack(last, wide, cross, turned)
    scale = 1.0 / spectra
    copies = []
    for b in range(part.shape[1] // BLOCK):
        rows = slice(b * BLOCK, (b + 1) * BLOCK)
        left = turned[rows, :]
        for p, right in enumerate((wide, cross)):
            term = jnp.dot(left, right[...], preferred_element_type=jnp.float32)
            done[p, rows, :] = (part[p, rows, :] + term) * scale
            copies.append(
                pltpu.make_async_copy(done.at[p, rows, :], out.at[0, p, rows, :], sem)
            )
            copies[-1].start()
    pltpu.make_async_copy(done, out.at[0], sem).wait()


def stream_device(voltages, pfb_coeff):
    n_inp = lax.axis_size("inp")
    n_tm = lax.axis_size("tm")
    channels = n_inp * n_tm
    in_rows = voltages.shape[0]
    taps, length = pfb_coeff.shape
    steps = voltages.shape[1] // (length * STEP)
    lines = 2 * channels
    heads = (taps + STEP - 1) // STEP
    table = jnp.asarray(split_table(channels, length))
    vmem = pl.BlockSpec(memory_space=pltpu.VMEM)
    hbm = pl.BlockSpec(memory_space=pl.ANY)
    bf16, f32 = jnp.bfloat16, jnp.float32
    carry = (taps - 1, lines, in_rows)
    inputs = n_inp * in_rows
    depth = n_tm * SPAN * 2 * STEP
    tiles = (channels * SPAN, 2 * STEP, in_rows)
    gram = (2, inputs, inputs)
    operands = [
        pltpu.VMEM((depth, inputs), bf16),
        pltpu.VMEM((depth, inputs), bf16),
        pltpu.VMEM((inputs, depth), bf16),
    ]
    part, last = pl.pallas_call(
        functools.partial(stream_kernel, n_inp, n_tm),
        out_shape=[pltpu.VMEM(gram, f32), pltpu.VMEM(tiles, bf16)],
        in_specs=[hbm, hbm, hbm],
        out_specs=[vmem, vmem],
        scratch_shapes=[
            pltpu.VMEM(pfb_coeff.shape, f32),
            pltpu.VMEM(table.shape, f32),
            pltpu.VMEM(voltages.shape, bf16),
            pltpu.VMEM((taps * lines, length), bf16),
            pltpu.VMEM((taps * lines, length), TINY),
            pltpu.VMEM((STEP // PART, PART * in_rows, length), TINY),
            pltpu.VMEM(carry, f32),
            pltpu.VMEM((2 * heads, lines * STEP, in_rows), f32),
            pltpu.VMEM(carry, f32),
            pltpu.VMEM(carry, f32),
            pltpu.VMEM((lines * STEP, in_rows), f32),
            pltpu.VMEM((steps, channels, 2 * STEP, in_rows), bf16),
            pltpu.VMEM((steps // SPAN - 1, *tiles), bf16),
            *operands,
            pltpu.SemaphoreType.DMA((2,)),
            pltpu.SemaphoreType.DMA((steps,)),
            pltpu.SemaphoreType.DMA,
            pltpu.SemaphoreType.DMA,
            pltpu.SemaphoreType.DMA,
            pltpu.SemaphoreType.DMA((steps // SPAN,)),
        ],
        compiler_params=pltpu.CompilerParams(
            collective_id=0, has_side_effects=True, vmem_limit_bytes=44 * 1024 * 1024
        ),
        name="stream",
    )(*(pltpu.with_memory_space_constraint(x, pltpu.HBM) for x in (voltages, pfb_coeff, table)))
    return pl.pallas_call(
        functools.partial(close_kernel, n_tm * steps * STEP),
        out_shape=jax.ShapeDtypeStruct((1, *gram), f32),
        in_specs=[vmem, vmem],
        out_specs=hbm,
        scratch_shapes=[*operands, pltpu.VMEM(gram, f32), pltpu.SemaphoreType.DMA],
        compiler_params=pltpu.CompilerParams(vmem_limit_bytes=24 * 1024 * 1024),
        name="close",
    )(part, last)


def per_device(voltages, pfb_coeff):
    if voltages.shape[0] % LANES == 0:
        return stream_device(voltages, pfb_coeff)
    return narrow_device(voltages, pfb_coeff)


def solution(mesh):
    return jax.shard_map(
        per_device,
        mesh=mesh,
        in_specs=(P("inp", "tm"), P()),
        out_specs=P(("inp", "tm"), None, None, None),
        check_vma=False,
    )
```

```python
import functools
import math

import jax
import jax.numpy as jnp
import numpy as np
from jax import lax
from jax.experimental import pallas as pl
from jax.experimental.pallas import tpu as pltpu
from jax.sharding import PartitionSpec as P

LANES = 128
ROWS = 16
GROUP = 8
CHUNK = 16
NT = (((1,), (1,)), ((), ()))


def dft_tables(channels, length):
    phase = np.arange(channels)[:, None] * np.arange(length)[None, :] % length
    angle = phase * (2.0 * math.pi / length)
    table = np.stack([np.cos(angle), -np.sin(angle)], axis=1) / math.sqrt(length)
    table = table.reshape(2 * channels, length).astype(np.float32)
    high = table.astype(jnp.bfloat16)
    low = (table - high.astype(np.float32)).astype(jnp.bfloat16)
    return np.concatenate([high, low], axis=0)


def channelize_kernel(
    n_inp, n_tm, volt, coef_in, table, out,
    slab, coef, high0, low0, high1, low1, stage, send,
    load_sem, tail_send, tail_recv, send_sem, recv_sem,
):
    in_rows = volt.shape[0]
    taps, length = coef_in.shape
    spec = volt.shape[1] // length
    lines = stage.shape[0] // CHUNK
    n_dev = n_inp * n_tm
    chunks = spec // CHUNK
    tail = (taps - 1) * length
    width = CHUNK * length
    a_tiles = in_rows // ROWS
    inp = lax.axis_index("inp")
    tm = lax.axis_index("tm")
    me = inp * n_tm + tm

    def load(q):
        return pltpu.make_async_copy(
            volt.at[:, pl.ds(pl.multiple_of(q * width, width), width)],
            slab.at[:, pl.ds(pl.multiple_of(tail + q * width, length), width)],
            load_sem.at[q],
        )

    load(0).start()
    load(1).start()

    barrier = pltpu.get_barrier_semaphore()

    def greet(d, _):
        other = lax.rem(me + d, n_dev)
        pl.semaphore_signal(
            barrier, inc=1, device_id=(other // n_tm, lax.rem(other, n_tm)),
            device_id_type=pl.DeviceIdType.MESH,
        )
        return _

    lax.fori_loop(1, n_dev, greet, 0)
    for j in range(taps):
        coef[j] = jnp.broadcast_to(coef_in[j : j + 1, :], (8, length))
    @pl.when(tm == 0)
    def _():
        def clear(e, _):
            slab[:, pl.ds(pl.multiple_of(e * length, length), length)] = jnp.zeros(
                (in_rows, length), slab.dtype
            )
            return _

        lax.fori_loop(0, taps - 1, clear, 0)

    f_high, f_low = (high0, high1), (low0, low1)

    def fir(first, tile, slot):
        row = pl.multiple_of(tile * ROWS, ROWS)
        for nt in range(length // LANES):
            lanes = pl.ds(nt * LANES, LANES)
            c = [coef[j, :, lanes] for j in range(taps)]
            low = [None] * GROUP
            high = [None] * GROUP
            for t in range(GROUP + taps - 1):
                col = pl.multiple_of((first + t) * length + nt * LANES, LANES)
                x = slab[pl.ds(row, ROWS), pl.ds(col, LANES)].astype(jnp.float32)
                x0, x1 = x[:8], x[8:]
                for i in range(max(0, t - taps + 1), min(GROUP - 1, t) + 1):
                    w = c[t - i]
                    if t == i:
                        low[i], high[i] = w * x0, w * x1
                    else:
                        low[i], high[i] = low[i] + w * x0, high[i] + w * x1
                i = t - taps + 1
                if i >= 0:
                    f = jnp.concatenate([low[i], high[i]], axis=0)
                    h = f.astype(jnp.bfloat16)
                    f_high[slot][i, pl.ds(row, ROWS), lanes] = h
                    f_low[slot][i, pl.ds(row, ROWS), lanes] = (
                        f - h.astype(jnp.float32)
                    ).astype(jnp.bfloat16)

    def dft(tile, slot):
        per = GROUP // a_tiles
        for u in range(per):
            i = tile * per + u
            r = lax.dot_general(table[...], f_high[slot][i], NT, preferred_element_type=jnp.float32)
            r2 = lax.dot_general(table[:lines], f_low[slot][i], NT, preferred_element_type=jnp.float32)
            stage[pl.ds(slot * GROUP + i, lines, stride=CHUNK), :] = r[:lines] + r[lines:] + r2

    def each(body):
        def step(tile, _):
            body(tile)
            return _

        lax.fori_loop(0, a_tiles, step, 0)

    def own(q):
        return pltpu.make_async_copy(send.at[q, me], place(out, q), recv_sem)

    def place(ref, q):
        first = pl.multiple_of(tm * spec + q * CHUNK, CHUNK)
        return ref.at[inp, :, pl.ds(first, CHUNK), :]

    def dispatch(q):
        def convert(d, _):
            rows = pl.ds(pl.multiple_of(d * 2 * CHUNK, 2 * CHUNK), 2 * CHUNK)
            send[q, d] = stage[rows, :].reshape(2, CHUNK, in_rows).astype(send.dtype)
            return _

        lax.fori_loop(0, n_dev, convert, 0)

        def post(d, _):
            other = lax.rem(me + d, n_dev)
            pltpu.make_async_remote_copy(
                src_ref=send.at[q, other], dst_ref=place(out, q),
                send_sem=send_sem, recv_sem=recv_sem,
                device_id=(other // n_tm, lax.rem(other, n_tm)),
                device_id_type=pl.DeviceIdType.MESH,
            ).start()
            return _

        lax.fori_loop(1, n_dev, post, 0)
        own(q).start()

    def chunk_of(k):
        return lax.rem(k + 1, chunks)

    load(0).wait()
    load(1).wait()
    for q in range(2, chunks):
        load(q).start()
    each(lambda tile: fir(chunk_of(0) * CHUNK, tile, 0))
    pl.semaphore_wait(barrier, n_dev - 1)

    history = pltpu.make_async_remote_copy(
        src_ref=volt.at[:, pl.ds(spec * length - tail, tail)],
        dst_ref=slab.at[:, pl.ds(0, tail)],
        send_sem=tail_send, recv_sem=tail_recv,
        device_id=(inp, lax.rem(tm + 1, n_tm)),
        device_id_type=pl.DeviceIdType.MESH,
    )

    @pl.when(tm < n_tm - 1)
    def _():
        history.start()

    def turn(k, carry):
        q = chunk_of(k)
        later = chunk_of(k + 1)

        def second(tile):
            dft(tile, 0)
            fir(q * CHUNK + GROUP, tile, 1)

        each(second)

        @pl.when(later > 0)
        def _():
            load(later).wait()

        @pl.when((later == 0) & (tm > 0))
        def _():
            history.wait_recv()

        def first(tile):
            dft(tile, 1)
            fir(later * CHUNK, tile, 0)

        each(first)
        dispatch(q)
        return carry

    lax.fori_loop(0, chunks - 1, turn, 0)

    def final(tile):
        dft(tile, 0)
        fir(GROUP, tile, 1)

    each(final)
    each(lambda tile: dft(tile, 1))
    dispatch(0)

    @pl.when(tm < n_tm - 1)
    def _():
        history.wait_send()

    sent = send.at[:, pl.ds(0, n_dev - 1)]
    pltpu.make_async_copy(sent, sent, send_sem).wait()
    pltpu.make_async_copy(out, out, recv_sem).wait()


def correlate_kernel(z_ref, o_ref, wide, turned, crossed):
    groups, _, spectra, in_rows = z_ref.shape
    block = o_ref.shape[2]

    @pl.when(pl.program_id(0) == 0)
    def _():
        for g in range(groups):
            cols = slice(g * in_rows, (g + 1) * in_rows)
            for p in range(2):
                part = z_ref[g, p]
                wide[p * spectra : (p + 1) * spectra, cols] = part
                flip = part.T
                turned[cols, p * spectra : (p + 1) * spectra] = flip
                crossed[cols, (1 - p) * spectra : (2 - p) * spectra] = flip if p else -flip

    rows = pl.ds(pl.multiple_of(pl.program_id(0) * block, block), block)
    scale = 1.0 / spectra
    o_ref[0, 0] = jnp.dot(turned[rows, :], wide[...], preferred_element_type=jnp.float32) * scale
    o_ref[0, 1] = jnp.dot(crossed[rows, :], wide[...], preferred_element_type=jnp.float32) * scale


def narrow_device(voltages, pfb_coeff):
    n_inp = lax.axis_size("inp")
    n_tm = lax.axis_size("tm")
    channels = n_inp * n_tm
    in_rows = voltages.shape[0]
    taps, length = pfb_coeff.shape
    spec = voltages.shape[1] // length
    lines = 2 * channels
    table = jnp.asarray(dft_tables(channels, length))
    vmem = pl.BlockSpec(memory_space=pltpu.VMEM)
    hbm = pl.BlockSpec(memory_space=pl.ANY)
    bf16 = jnp.bfloat16
    received = pl.pallas_call(
        functools.partial(channelize_kernel, n_inp, n_tm),
        out_shape=jax.ShapeDtypeStruct((n_inp, 2, n_tm * spec, in_rows), bf16),
        in_specs=[hbm, vmem, vmem],
        out_specs=hbm,
        scratch_shapes=[
            pltpu.VMEM((in_rows, (spec + taps - 1) * length), bf16),
            pltpu.VMEM((taps, 8, length), jnp.float32),
            pltpu.VMEM((GROUP, in_rows, length), bf16),
            pltpu.VMEM((GROUP, in_rows, length), bf16),
            pltpu.VMEM((GROUP, in_rows, length), bf16),
            pltpu.VMEM((GROUP, in_rows, length), bf16),
            pltpu.VMEM((lines * CHUNK, in_rows), jnp.float32),
            pltpu.VMEM((spec // CHUNK, channels, 2, CHUNK, in_rows), bf16),
            pltpu.SemaphoreType.DMA((spec // CHUNK,)),
            pltpu.SemaphoreType.DMA,
            pltpu.SemaphoreType.DMA,
            pltpu.SemaphoreType.DMA,
            pltpu.SemaphoreType.DMA,
        ],
        compiler_params=pltpu.CompilerParams(
            collective_id=0, has_side_effects=True, vmem_limit_bytes=60 * 1024 * 1024
        ),
        name="channelize",
    )(voltages, pfb_coeff, table)
    inputs = n_inp * in_rows
    spectra = n_tm * spec
    block = min(256, inputs)
    return pl.pallas_call(
        correlate_kernel,
        grid=(inputs // block,),
        out_shape=jax.ShapeDtypeStruct((1, 2, inputs, inputs), jnp.float32),
        in_specs=[pl.BlockSpec(received.shape, lambda i: (0, 0, 0, 0))],
        out_specs=pl.BlockSpec((1, 2, block, inputs), lambda i: (0, 0, i, 0)),
        scratch_shapes=[
            pltpu.VMEM((2 * spectra, inputs), bf16),
            pltpu.VMEM((inputs, 2 * spectra), bf16),
            pltpu.VMEM((inputs, 2 * spectra), bf16),
        ],
        compiler_params=pltpu.CompilerParams(vmem_limit_bytes=60 * 1024 * 1024),
        name="correlate",
    )(received)


STEP = 8
PART = 4
SPAN = 4
BLOCK = 256
AHEAD = 3
TINY = jnp.float8_e5m2
LIFT = 2.0**12
GAIN = 2.0**38


def split_table(channels, length):
    phase = np.arange(channels)[:, None] * np.arange(length)[None, :] % length
    angle = phase * (2.0 * math.pi / length)
    table = np.stack([np.cos(angle), -np.sin(angle)], axis=1) / math.sqrt(length)
    return table.reshape(2 * channels, length).astype(np.float32)


def stream_kernel(
    n_inp, n_tm, volt, coef_from, table_from, part, landed,
    coef_in, table, slab, taps_table, low_table, thin, acc, head, tail_out, tail_in, stage, send,
    wide, cross, turned, small_sem, load_sem, tail_send, tail_recv, send_sem, recv_sem,
):
    in_rows = volt.shape[0]
    taps, length = coef_from.shape
    steps = volt.shape[1] // (length * STEP)
    lines = table_from.shape[0]
    n_dev = n_inp * n_tm
    width = STEP * length
    inp = lax.axis_index("inp")
    tm = lax.axis_index("tm")
    me = inp * n_tm + tm
    heads = (taps + STEP - 1) // STEP
    turn = steps - heads

    def load(i):
        cols = pl.ds(pl.multiple_of(i * width, width), width)
        return pltpu.make_async_copy(volt.at[:, cols], slab.at[:, cols], load_sem.at[i])

    small = [
        pltpu.make_async_copy(source, target, small_sem.at[n])
        for n, (source, target) in enumerate(((coef_from, coef_in), (table_from, table)))
    ]
    for copy in small:
        copy.start()
    for t in range(AHEAD):
        load((t + heads) % steps).start()

    barrier = pltpu.get_barrier_semaphore()

    def greet(d, _):
        other = lax.rem(me + d, n_dev)
        pl.semaphore_signal(
            barrier, inc=1, device_id=(other // n_tm, lax.rem(other, n_tm)),
            device_id_type=pl.DeviceIdType.MESH,
        )
        return _

    lax.fori_loop(1, n_dev, greet, 0)
    for copy in small:
        copy.wait()

    def build(j, _):
        full = table[...] * coef_in[pl.ds(j, 1), :] * GAIN
        high = full.astype(jnp.bfloat16)
        rows = pl.ds(pl.multiple_of(j * lines, lines), lines)
        taps_table[rows, :] = high
        low_table[rows, :] = ((full - high.astype(jnp.float32)) / LIFT).astype(TINY)
        return _

    lax.fori_loop(0, taps, build, 0)
    acc[...] = jnp.zeros(acc.shape, acc.dtype)

    half = n_inp // 2
    side = inp // half
    fars = [(1 - side) * half + lax.rem(inp + d, half) for d in range(half)]
    nears = [side * half + lax.rem(inp + d, half) for d in range(half)]
    cores = [lax.rem(tm + d, n_tm) for d in range(n_tm)]

    def dispatch(i):
        send[i] = (stage[...] * (1.0 / GAIN)).reshape(n_dev, 2 * STEP, in_rows).astype(send.dtype)
        group = i // SPAN
        target = landed.at[group, me * SPAN + lax.rem(i, SPAN)]

        def post(inp2, tm2):
            pltpu.make_async_remote_copy(
                src_ref=send.at[i, inp2 * n_tm + tm2], dst_ref=target,
                send_sem=send_sem, recv_sem=recv_sem.at[group],
                device_id=(inp2, tm2), device_id_type=pl.DeviceIdType.MESH,
            ).start()

        for row in fars:
            for core in cores:
                post(row, core)
        for d, row in enumerate(nears):
            for core in cores[d == 0 :]:
                post(row, core)
        target[...] = send[i, me]

    def advance(i, skip=0):
        first = i * width
        for h in range(STEP // PART):
            start = max(skip - h * PART, 0)
            used = min(PART + taps - 1 - start, taps) * lines
            x = jnp.concatenate(
                [
                    slab[:, pl.ds(pl.multiple_of(first + (h * PART + u) * length, length), length)]
                    for u in range(PART)
                ],
                axis=0,
            )
            thin[h] = (x.astype(jnp.float32) * LIFT).astype(TINY)
            high = lax.dot_general(taps_table[:used, :], x, NT, preferred_element_type=jnp.float32)
            low = lax.dot_general(low_table[:used, :], thin[h], NT, preferred_element_type=jnp.float32)
            for k in range(start, taps + PART - 1):
                total = acc[k] if k < taps - 1 else None
                for u in range(PART):
                    j = u + taps - 1 - k
                    if 0 <= j < taps:
                        spot = (slice(j * lines, (j + 1) * lines), slice(u * in_rows, (u + 1) * in_rows))
                        term = high[spot] + low[spot]
                        total = term if total is None else total + term
                if k < PART:
                    stage[pl.ds(h * PART + k, lines, stride=STEP), :] = total
                else:
                    acc[k - PART] = total

    def finish(q):
        for k in range(STEP):
            rows = pl.ds(k, lines, stride=STEP)
            total = head[q, rows, :]
            s = q * STEP + k
            stage[rows, :] = total + tail_in[s] if s < taps - 1 else total
        dispatch(q)

    history = pltpu.make_async_remote_copy(
        src_ref=tail_out, dst_ref=tail_in, send_sem=tail_send, recv_sem=tail_recv,
        device_id=(inp, lax.rem(tm + 1, n_tm)), device_id_type=pl.DeviceIdType.MESH,
    )

    for t in range(heads):
        load(t + heads).wait()
        load(t + heads + AHEAD).start()
        advance(t + heads, (heads - t) * STEP)
    pl.semaphore_wait(barrier, n_dev - 1)

    def work(t, carry):
        i = lax.rem(t + heads, steps)

        @pl.when(t < steps)
        def _():
            load(i).wait()

        @pl.when(t < steps - AHEAD)
        def _():
            load(lax.rem(i + AHEAD, steps)).start()

        @pl.when(t == turn)
        def _():
            tail_out[...] = acc[...]
            acc[...] = jnp.zeros(acc.shape, acc.dtype)

            @pl.when(tm < n_tm - 1)
            def _():
                history.start()

        advance(i)

        @pl.when(i < heads)
        def _():
            head[i] = stage[...]

        @pl.when(i >= heads)
        def _():
            dispatch(i)

        return carry

    lax.fori_loop(heads, steps + heads, work, 0)

    def arrive(group):
        came = landed.at[group, pl.ds(0, (n_dev - 1) * SPAN)]
        pltpu.make_async_copy(came, came, recv_sem.at[group]).wait()

    def fold(group):
        arrive(group)
        pack(landed.at[group], wide, cross, turned)

        def block(b, carry):
            rows = pl.ds(pl.multiple_of(b * BLOCK, BLOCK), BLOCK)
            left = turned[rows, :]
            for p, right in enumerate((wide, cross)):
                term = jnp.dot(left, right[...], preferred_element_type=jnp.float32)
                part[p, rows, :] = term if group == 1 else part[p, rows, :] + term
            return carry

        lax.fori_loop(0, part.shape[1] // BLOCK, block, 0)

    for group in range(1, steps // SPAN - 1):
        fold(group)

    @pl.when(tm > 0)
    def _():
        history.wait_recv()

    @pl.when(tm == 0)
    def _():
        tail_in[...] = jnp.zeros(tail_in.shape, tail_in.dtype)

    for q in range(heads):
        finish(q)
    fold(steps // SPAN - 1)

    @pl.when(tm < n_tm - 1)
    def _():
        history.wait_send()

    sent = send.at[:, pl.ds(0, n_dev - 1)]
    pltpu.make_async_copy(sent, sent, send_sem).wait()
    arrive(0)


def pack(source, wide, cross, turned):
    depth, inputs = wide.shape
    tiles, pair, in_rows = source.shape
    span = depth // pair
    for g in range(inputs // in_rows):
        cols = slice(g * in_rows, (g + 1) * in_rows)
        piece = source[g * span : (g + 1) * span]
        flat = piece.reshape(depth, in_rows)
        wide[:, cols] = flat
        turned[cols, :] = flat.T
        full = piece.astype(jnp.float32)
        swap = jnp.concatenate([-full[:, pair // 2 :], full[:, : pair // 2]], axis=1)
        cross[:, cols] = swap.astype(piece.dtype).reshape(depth, in_rows)


def close_kernel(spectra, part, landed, out, wide, cross, turned, done, sem):
    pack(landed.at[0], wide, cross, turned)
    scale = 1.0 / spectra
    copies = []
    for b in range(part.shape[1] // BLOCK):
        rows = slice(b * BLOCK, (b + 1) * BLOCK)
        left = turned[rows, :]
        for p, right in enumerate((wide, cross)):
            term = jnp.dot(left, right[...], preferred_element_type=jnp.float32)
            done[p, rows, :] = (part[p, rows, :] + term) * scale
            copies.append(
                pltpu.make_async_copy(done.at[p, rows, :], out.at[0, p, rows, :], sem)
            )
            copies[-1].start()
    pltpu.make_async_copy(done, out.at[0], sem).wait()


def stream_device(voltages, pfb_coeff):
    n_inp = lax.axis_size("inp")
    n_tm = lax.axis_size("tm")
    channels = n_inp * n_tm
    in_rows = voltages.shape[0]
    taps, length = pfb_coeff.shape
    steps = voltages.shape[1] // (length * STEP)
    lines = 2 * channels
    heads = (taps + STEP - 1) // STEP
    table = jnp.asarray(split_table(channels, length))
    vmem = pl.BlockSpec(memory_space=pltpu.VMEM)
    hbm = pl.BlockSpec(memory_space=pl.ANY)
    bf16, f32 = jnp.bfloat16, jnp.float32
    carry = (taps - 1, lines, in_rows)
    inputs = n_inp * in_rows
    depth = n_tm * SPAN * 2 * STEP
    tiles = (steps // SPAN, channels * SPAN, 2 * STEP, in_rows)
    gram = (2, inputs, inputs)
    operands = [
        pltpu.VMEM((depth, inputs), bf16),
        pltpu.VMEM((depth, inputs), bf16),
        pltpu.VMEM((inputs, depth), bf16),
    ]
    part, landed = pl.pallas_call(
        functools.partial(stream_kernel, n_inp, n_tm),
        out_shape=[pltpu.VMEM(gram, f32), pltpu.VMEM(tiles, bf16)],
        in_specs=[hbm, hbm, hbm],
        out_specs=[vmem, vmem],
        scratch_shapes=[
            pltpu.VMEM(pfb_coeff.shape, f32),
            pltpu.VMEM(table.shape, f32),
            pltpu.VMEM(voltages.shape, bf16),
            pltpu.VMEM((taps * lines, length), bf16),
            pltpu.VMEM((taps * lines, length), TINY),
            pltpu.VMEM((STEP // PART, PART * in_rows, length), TINY),
            pltpu.VMEM(carry, f32),
            pltpu.VMEM((heads, lines * STEP, in_rows), f32),
            pltpu.VMEM(carry, f32),
            pltpu.VMEM(carry, f32),
            pltpu.VMEM((lines * STEP, in_rows), f32),
            pltpu.VMEM((steps, channels, 2 * STEP, in_rows), bf16),
            *operands,
            pltpu.SemaphoreType.DMA((2,)),
            pltpu.SemaphoreType.DMA((steps,)),
            pltpu.SemaphoreType.DMA,
            pltpu.SemaphoreType.DMA,
            pltpu.SemaphoreType.DMA,
            pltpu.SemaphoreType.DMA((steps // SPAN,)),
        ],
        compiler_params=pltpu.CompilerParams(
            collective_id=0, has_side_effects=True, vmem_limit_bytes=44 * 1024 * 1024
        ),
        name="stream",
    )(*(pltpu.with_memory_space_constraint(x, pltpu.HBM) for x in (voltages, pfb_coeff, table)))
    return pl.pallas_call(
        functools.partial(close_kernel, n_tm * steps * STEP),
        out_shape=jax.ShapeDtypeStruct((1, *gram), f32),
        in_specs=[vmem, vmem],
        out_specs=hbm,
        scratch_shapes=[*operands, pltpu.VMEM(gram, f32), pltpu.SemaphoreType.DMA],
        compiler_params=pltpu.CompilerParams(vmem_limit_bytes=24 * 1024 * 1024),
        name="close",
    )(part, landed)


def per_device(voltages, pfb_coeff):
    if voltages.shape[0] % LANES == 0:
        return stream_device(voltages, pfb_coeff)
    return narrow_device(voltages, pfb_coeff)


def solution(mesh):
    return jax.shard_map(
        per_device,
        mesh=mesh,
        in_specs=(P("inp", "tm"), P()),
        out_specs=P(("inp", "tm"), None, None, None),
        check_vma=False,
    )
```

```python
import functools
import math

import jax
import jax.numpy as jnp
import numpy as np
from jax import lax
from jax.experimental import pallas as pl
from jax.experimental.pallas import tpu as pltpu
from jax.sharding import PartitionSpec as P

LANES = 128
ROWS = 16
GROUP = 8
CHUNK = 16
NT = (((1,), (1,)), ((), ()))


def dft_tables(channels, length):
    phase = np.arange(channels)[:, None] * np.arange(length)[None, :] % length
    angle = phase * (2.0 * math.pi / length)
    table = np.stack([np.cos(angle), -np.sin(angle)], axis=1) / math.sqrt(length)
    table = table.reshape(2 * channels, length).astype(np.float32)
    high = table.astype(jnp.bfloat16)
    low = (table - high.astype(np.float32)).astype(jnp.bfloat16)
    return np.concatenate([high, low], axis=0)


def channelize_kernel(
    n_inp, n_tm, volt, coef_in, table, out,
    slab, coef, high0, low0, high1, low1, stage, send,
    load_sem, tail_send, tail_recv, send_sem, recv_sem,
):
    in_rows = volt.shape[0]
    taps, length = coef_in.shape
    spec = volt.shape[1] // length
    lines = stage.shape[0] // CHUNK
    n_dev = n_inp * n_tm
    chunks = spec // CHUNK
    tail = (taps - 1) * length
    width = CHUNK * length
    a_tiles = in_rows // ROWS
    inp = lax.axis_index("inp")
    tm = lax.axis_index("tm")
    me = inp * n_tm + tm

    def load(q):
        return pltpu.make_async_copy(
            volt.at[:, pl.ds(pl.multiple_of(q * width, width), width)],
            slab.at[:, pl.ds(pl.multiple_of(tail + q * width, length), width)],
            load_sem.at[q],
        )

    load(0).start()
    load(1).start()

    barrier = pltpu.get_barrier_semaphore()

    def greet(d, _):
        other = lax.rem(me + d, n_dev)
        pl.semaphore_signal(
            barrier, inc=1, device_id=(other // n_tm, lax.rem(other, n_tm)),
            device_id_type=pl.DeviceIdType.MESH,
        )
        return _

    lax.fori_loop(1, n_dev, greet, 0)
    for j in range(taps):
        coef[j] = jnp.broadcast_to(coef_in[j : j + 1, :], (8, length))
    @pl.when(tm == 0)
    def _():
        def clear(e, _):
            slab[:, pl.ds(pl.multiple_of(e * length, length), length)] = jnp.zeros(
                (in_rows, length), slab.dtype
            )
            return _

        lax.fori_loop(0, taps - 1, clear, 0)

    f_high, f_low = (high0, high1), (low0, low1)

    def fir(first, tile, slot):
        row = pl.multiple_of(tile * ROWS, ROWS)
        for nt in range(length // LANES):
            lanes = pl.ds(nt * LANES, LANES)
            c = [coef[j, :, lanes] for j in range(taps)]
            low = [None] * GROUP
            high = [None] * GROUP
            for t in range(GROUP + taps - 1):
                col = pl.multiple_of((first + t) * length + nt * LANES, LANES)
                x = slab[pl.ds(row, ROWS), pl.ds(col, LANES)].astype(jnp.float32)
                x0, x1 = x[:8], x[8:]
                for i in range(max(0, t - taps + 1), min(GROUP - 1, t) + 1):
                    w = c[t - i]
                    if t == i:
                        low[i], high[i] = w * x0, w * x1
                    else:
                        low[i], high[i] = low[i] + w * x0, high[i] + w * x1
                i = t - taps + 1
                if i >= 0:
                    f = jnp.concatenate([low[i], high[i]], axis=0)
                    h = f.astype(jnp.bfloat16)
                    f_high[slot][i, pl.ds(row, ROWS), lanes] = h
                    f_low[slot][i, pl.ds(row, ROWS), lanes] = (
                        f - h.astype(jnp.float32)
                    ).astype(jnp.bfloat16)

    def dft(tile, slot):
        per = GROUP // a_tiles
        for u in range(per):
            i = tile * per + u
            r = lax.dot_general(table[...], f_high[slot][i], NT, preferred_element_type=jnp.float32)
            r2 = lax.dot_general(table[:lines], f_low[slot][i], NT, preferred_element_type=jnp.float32)
            stage[pl.ds(slot * GROUP + i, lines, stride=CHUNK), :] = r[:lines] + r[lines:] + r2

    def each(body):
        def step(tile, _):
            body(tile)
            return _

        lax.fori_loop(0, a_tiles, step, 0)

    def own(q):
        return pltpu.make_async_copy(send.at[q, me], place(out, q), recv_sem)

    def place(ref, q):
        first = pl.multiple_of(tm * spec + q * CHUNK, CHUNK)
        return ref.at[inp, :, pl.ds(first, CHUNK), :]

    def dispatch(q):
        def convert(d, _):
            rows = pl.ds(pl.multiple_of(d * 2 * CHUNK, 2 * CHUNK), 2 * CHUNK)
            send[q, d] = stage[rows, :].reshape(2, CHUNK, in_rows).astype(send.dtype)
            return _

        lax.fori_loop(0, n_dev, convert, 0)

        def post(d, _):
            other = lax.rem(me + d, n_dev)
            pltpu.make_async_remote_copy(
                src_ref=send.at[q, other], dst_ref=place(out, q),
                send_sem=send_sem, recv_sem=recv_sem,
                device_id=(other // n_tm, lax.rem(other, n_tm)),
                device_id_type=pl.DeviceIdType.MESH,
            ).start()
            return _

        lax.fori_loop(1, n_dev, post, 0)
        own(q).start()

    def chunk_of(k):
        return lax.rem(k + 1, chunks)

    load(0).wait()
    load(1).wait()
    for q in range(2, chunks):
        load(q).start()
    each(lambda tile: fir(chunk_of(0) * CHUNK, tile, 0))
    pl.semaphore_wait(barrier, n_dev - 1)

    history = pltpu.make_async_remote_copy(
        src_ref=volt.at[:, pl.ds(spec * length - tail, tail)],
        dst_ref=slab.at[:, pl.ds(0, tail)],
        send_sem=tail_send, recv_sem=tail_recv,
        device_id=(inp, lax.rem(tm + 1, n_tm)),
        device_id_type=pl.DeviceIdType.MESH,
    )

    @pl.when(tm < n_tm - 1)
    def _():
        history.start()

    def turn(k, carry):
        q = chunk_of(k)
        later = chunk_of(k + 1)

        def second(tile):
            dft(tile, 0)
            fir(q * CHUNK + GROUP, tile, 1)

        each(second)

        @pl.when(later > 0)
        def _():
            load(later).wait()

        @pl.when((later == 0) & (tm > 0))
        def _():
            history.wait_recv()

        def first(tile):
            dft(tile, 1)
            fir(later * CHUNK, tile, 0)

        each(first)
        dispatch(q)
        return carry

    lax.fori_loop(0, chunks - 1, turn, 0)

    def final(tile):
        dft(tile, 0)
        fir(GROUP, tile, 1)

    each(final)
    each(lambda tile: dft(tile, 1))
    dispatch(0)

    @pl.when(tm < n_tm - 1)
    def _():
        history.wait_send()

    sent = send.at[:, pl.ds(0, n_dev - 1)]
    pltpu.make_async_copy(sent, sent, send_sem).wait()
    pltpu.make_async_copy(out, out, recv_sem).wait()


def correlate_kernel(z_ref, o_ref, wide, turned, crossed):
    groups, _, spectra, in_rows = z_ref.shape
    block = o_ref.shape[2]

    @pl.when(pl.program_id(0) == 0)
    def _():
        for g in range(groups):
            cols = slice(g * in_rows, (g + 1) * in_rows)
            for p in range(2):
                part = z_ref[g, p]
                wide[p * spectra : (p + 1) * spectra, cols] = part
                flip = part.T
                turned[cols, p * spectra : (p + 1) * spectra] = flip
                crossed[cols, (1 - p) * spectra : (2 - p) * spectra] = flip if p else -flip

    rows = pl.ds(pl.multiple_of(pl.program_id(0) * block, block), block)
    scale = 1.0 / spectra
    o_ref[0, 0] = jnp.dot(turned[rows, :], wide[...], preferred_element_type=jnp.float32) * scale
    o_ref[0, 1] = jnp.dot(crossed[rows, :], wide[...], preferred_element_type=jnp.float32) * scale


def narrow_device(voltages, pfb_coeff):
    n_inp = lax.axis_size("inp")
    n_tm = lax.axis_size("tm")
    channels = n_inp * n_tm
    in_rows = voltages.shape[0]
    taps, length = pfb_coeff.shape
    spec = voltages.shape[1] // length
    lines = 2 * channels
    table = jnp.asarray(dft_tables(channels, length))
    vmem = pl.BlockSpec(memory_space=pltpu.VMEM)
    hbm = pl.BlockSpec(memory_space=pl.ANY)
    bf16 = jnp.bfloat16
    received = pl.pallas_call(
        functools.partial(channelize_kernel, n_inp, n_tm),
        out_shape=jax.ShapeDtypeStruct((n_inp, 2, n_tm * spec, in_rows), bf16),
        in_specs=[hbm, vmem, vmem],
        out_specs=hbm,
        scratch_shapes=[
            pltpu.VMEM((in_rows, (spec + taps - 1) * length), bf16),
            pltpu.VMEM((taps, 8, length), jnp.float32),
            pltpu.VMEM((GROUP, in_rows, length), bf16),
            pltpu.VMEM((GROUP, in_rows, length), bf16),
            pltpu.VMEM((GROUP, in_rows, length), bf16),
            pltpu.VMEM((GROUP, in_rows, length), bf16),
            pltpu.VMEM((lines * CHUNK, in_rows), jnp.float32),
            pltpu.VMEM((spec // CHUNK, channels, 2, CHUNK, in_rows), bf16),
            pltpu.SemaphoreType.DMA((spec // CHUNK,)),
            pltpu.SemaphoreType.DMA,
            pltpu.SemaphoreType.DMA,
            pltpu.SemaphoreType.DMA,
            pltpu.SemaphoreType.DMA,
        ],
        compiler_params=pltpu.CompilerParams(
            collective_id=0, has_side_effects=True, vmem_limit_bytes=60 * 1024 * 1024
        ),
        name="channelize",
    )(voltages, pfb_coeff, table)
    inputs = n_inp * in_rows
    spectra = n_tm * spec
    block = min(256, inputs)
    return pl.pallas_call(
        correlate_kernel,
        grid=(inputs // block,),
        out_shape=jax.ShapeDtypeStruct((1, 2, inputs, inputs), jnp.float32),
        in_specs=[pl.BlockSpec(received.shape, lambda i: (0, 0, 0, 0))],
        out_specs=pl.BlockSpec((1, 2, block, inputs), lambda i: (0, 0, i, 0)),
        scratch_shapes=[
            pltpu.VMEM((2 * spectra, inputs), bf16),
            pltpu.VMEM((inputs, 2 * spectra), bf16),
            pltpu.VMEM((inputs, 2 * spectra), bf16),
        ],
        compiler_params=pltpu.CompilerParams(vmem_limit_bytes=60 * 1024 * 1024),
        name="correlate",
    )(received)


STEP = 8
PART = 4
SPAN = 4
BLOCK = 256
AHEAD = 3
TINY = jnp.float8_e5m2
LIFT = 2.0**12
GAIN = 2.0**38


def split_table(channels, length):
    phase = np.arange(channels)[:, None] * np.arange(length)[None, :] % length
    angle = phase * (2.0 * math.pi / length)
    table = np.stack([np.cos(angle), -np.sin(angle)], axis=1) / math.sqrt(length)
    return table.reshape(2 * channels, length).astype(np.float32)


def stream_kernel(
    n_inp, n_tm, volt, coef_from, table_from, part, landed,
    coef_in, table, slab, taps_table, low_table, thin, acc, head, tail_out, tail_in, stage, send,
    wide, cross, turned, small_sem, load_sem, tail_send, tail_recv, send_sem, recv_sem,
):
    in_rows = volt.shape[0]
    taps, length = coef_from.shape
    steps = volt.shape[1] // (length * STEP)
    lines = table_from.shape[0]
    n_dev = n_inp * n_tm
    width = STEP * length
    inp = lax.axis_index("inp")
    tm = lax.axis_index("tm")
    me = inp * n_tm + tm
    heads = (taps + STEP - 1) // STEP
    origin = steps // 2
    turn = steps - origin

    def load(i):
        cols = pl.ds(pl.multiple_of(i * width, width), width)
        return pltpu.make_async_copy(volt.at[:, cols], slab.at[:, cols], load_sem.at[i])

    small = [
        pltpu.make_async_copy(source, target, small_sem.at[n])
        for n, (source, target) in enumerate(((coef_from, coef_in), (table_from, table)))
    ]
    for copy in small:
        copy.start()
    for t in range(AHEAD):
        load((t + origin) % steps).start()

    barrier = pltpu.get_barrier_semaphore()

    def greet(d, _):
        other = lax.rem(me + d, n_dev)
        pl.semaphore_signal(
            barrier, inc=1, device_id=(other // n_tm, lax.rem(other, n_tm)),
            device_id_type=pl.DeviceIdType.MESH,
        )
        return _

    lax.fori_loop(1, n_dev, greet, 0)
    acc[...] = jnp.zeros(acc.shape, acc.dtype)
    for copy in small:
        copy.wait()

    early = min(STEP + taps - 1 - heads * STEP, taps)

    def build(j, _):
        full = table[...] * coef_in[pl.ds(j, 1), :] * GAIN
        high = full.astype(jnp.bfloat16)
        rows = pl.ds(j * lines if isinstance(j, int) else pl.multiple_of(j * lines, lines), lines)
        taps_table[rows, :] = high
        low_table[rows, :] = ((full - high.astype(jnp.float32)) / LIFT).astype(TINY)
        return _

    lax.fori_loop(0, early, build, 0)

    half = n_inp // 2
    side = inp // half
    fars = [(1 - side) * half + lax.rem(inp + d, half) for d in range(half)]
    nears = [side * half + lax.rem(inp + d, half) for d in range(half)]
    cores = [lax.rem(tm + d, n_tm) for d in range(n_tm)]

    def dispatch(i, place):
        send[i] = (stage[...] * (1.0 / GAIN)).reshape(n_dev, 2 * STEP, in_rows).astype(send.dtype)
        group = place // SPAN
        target = landed.at[group, me * SPAN + place % SPAN]

        def post(inp2, tm2):
            pltpu.make_async_remote_copy(
                src_ref=send.at[i, inp2 * n_tm + tm2], dst_ref=target,
                send_sem=send_sem, recv_sem=recv_sem.at[group],
                device_id=(inp2, tm2), device_id_type=pl.DeviceIdType.MESH,
            ).start()

        for row in fars:
            for core in cores:
                post(row, core)
        for d, row in enumerate(nears):
            for core in cores[d == 0 :]:
                post(row, core)
        target[...] = send[i, me]

    def advance(i, skip=0, stop=STEP + taps - 1):
        first = i * width
        for h in range(STEP // PART):
            start = max(skip - h * PART, 0)
            end = min(stop - h * PART, PART + taps - 1)
            base = max(taps - end, 0) * lines
            used = min(PART + taps - 1 - start, taps) * lines
            x = jnp.concatenate(
                [
                    slab[:, pl.ds(pl.multiple_of(first + (h * PART + u) * length, length), length)]
                    for u in range(PART)
                ],
                axis=0,
            )
            thin[h] = (x.astype(jnp.float32) * LIFT).astype(TINY)
            high = lax.dot_general(taps_table[base:used, :], x, NT, preferred_element_type=jnp.float32)
            low = lax.dot_general(low_table[base:used, :], thin[h], NT, preferred_element_type=jnp.float32)
            for k in range(start, end):
                total = acc[k] if k < taps - 1 else None
                for u in range(PART):
                    j = u + taps - 1 - k
                    if 0 <= j < taps:
                        spot = (slice(j * lines - base, (j + 1) * lines - base), slice(u * in_rows, (u + 1) * in_rows))
                        term = high[spot] + low[spot]
                        total = term if total is None else total + term
                if k < PART:
                    stage[pl.ds(h * PART + k, lines, stride=STEP), :] = total
                else:
                    acc[k - PART] = total

    def finish(q):
        for k in range(STEP):
            rows = pl.ds(k, lines, stride=STEP)
            total = head[q, rows, :]
            s = q * STEP + k
            stage[rows, :] = total + tail_in[s] if s < taps - 1 else total
        dispatch(q, steps - heads + q)

    history = pltpu.make_async_remote_copy(
        src_ref=tail_out, dst_ref=tail_in, send_sem=tail_send, recv_sem=tail_recv,
        device_id=(inp, lax.rem(tm + 1, n_tm)), device_id_type=pl.DeviceIdType.MESH,
    )

    for t in range(heads):
        load(t + origin).wait()
        load((t + origin + AHEAD) % steps).start()
        advance(t + origin, (heads - t) * STEP)
        if t == 0:
            for j in range(early, taps):
                build(j, None)
    load(origin + heads).wait()
    load((origin + heads + AHEAD) % steps).start()
    pl.semaphore_wait(barrier, n_dev - 1)
    advance(origin + heads, 0, STEP)
    dispatch(origin + heads, 0)
    advance(origin + heads, STEP)

    def work(t, carry):
        i = lax.rem(t + origin, steps)

        @pl.when(t < steps)
        def _():
            load(i).wait()

        @pl.when(t < steps - AHEAD)
        def _():
            load(lax.rem(i + AHEAD, steps)).start()

        @pl.when(t == turn)
        def _():
            tail_out[...] = acc[...]
            acc[...] = jnp.zeros(acc.shape, acc.dtype)

            @pl.when(tm < n_tm - 1)
            def _():
                history.start()

        advance(i)

        @pl.when(i < heads)
        def _():
            head[i] = stage[...]

        @pl.when(i >= heads)
        def _():
            dispatch(i, lax.rem(i + steps - 2 * heads - origin, steps - heads))

        return carry

    lax.fori_loop(heads + 1, steps + heads, work, 0)

    @pl.when(tm > 0)
    def _():
        history.wait_recv()

    @pl.when(tm == 0)
    def _():
        tail_in[...] = jnp.zeros(tail_in.shape, tail_in.dtype)

    for q in range(heads):
        finish(q)

    def arrive(group):
        came = landed.at[group, pl.ds(0, (n_dev - 1) * SPAN)]
        pltpu.make_async_copy(came, came, recv_sem.at[group]).wait()

    def fold(group):
        arrive(group)
        pack(landed.at[group], wide, cross, turned)

        def block(b, carry):
            rows = pl.ds(pl.multiple_of(b * BLOCK, BLOCK), BLOCK)
            left = turned[rows, :]
            for p, right in enumerate((wide, cross)):
                term = jnp.dot(left, right[...], preferred_element_type=jnp.float32)
                part[p, rows, :] = term if group == 0 else part[p, rows, :] + term
            return carry

        lax.fori_loop(0, part.shape[1] // BLOCK, block, 0)

    for group in range(steps // SPAN - 1):
        fold(group)

    @pl.when(tm < n_tm - 1)
    def _():
        history.wait_send()

    sent = send.at[:, pl.ds(0, n_dev - 1)]
    pltpu.make_async_copy(sent, sent, send_sem).wait()
    arrive(steps // SPAN - 1)


def pack(source, wide, cross, turned):
    depth, inputs = wide.shape
    tiles, pair, in_rows = source.shape
    span = depth // pair
    for g in range(inputs // in_rows):
        cols = slice(g * in_rows, (g + 1) * in_rows)
        piece = source[g * span : (g + 1) * span]
        flat = piece.reshape(depth, in_rows)
        wide[:, cols] = flat
        turned[cols, :] = flat.T
        full = piece.astype(jnp.float32)
        swap = jnp.concatenate([-full[:, pair // 2 :], full[:, : pair // 2]], axis=1)
        cross[:, cols] = swap.astype(piece.dtype).reshape(depth, in_rows)


def close_kernel(spectra, part, landed, out, wide, cross, turned, done, sem):
    pack(landed.at[landed.shape[0] - 1], wide, cross, turned)
    scale = 1.0 / spectra
    copies = []
    for b in range(part.shape[1] // BLOCK):
        rows = slice(b * BLOCK, (b + 1) * BLOCK)
        left = turned[rows, :]
        for p, right in enumerate((wide, cross)):
            term = jnp.dot(left, right[...], preferred_element_type=jnp.float32)
            done[p, rows, :] = (part[p, rows, :] + term) * scale
            copies.append(
                pltpu.make_async_copy(done.at[p, rows, :], out.at[0, p, rows, :], sem)
            )
            copies[-1].start()
    pltpu.make_async_copy(done, out.at[0], sem).wait()


def stream_device(voltages, pfb_coeff):
    n_inp = lax.axis_size("inp")
    n_tm = lax.axis_size("tm")
    channels = n_inp * n_tm
    in_rows = voltages.shape[0]
    taps, length = pfb_coeff.shape
    steps = voltages.shape[1] // (length * STEP)
    lines = 2 * channels
    heads = (taps + STEP - 1) // STEP
    table = jnp.asarray(split_table(channels, length))
    vmem = pl.BlockSpec(memory_space=pltpu.VMEM)
    hbm = pl.BlockSpec(memory_space=pl.ANY)
    bf16, f32 = jnp.bfloat16, jnp.float32
    carry = (taps - 1, lines, in_rows)
    inputs = n_inp * in_rows
    depth = n_tm * SPAN * 2 * STEP
    tiles = (steps // SPAN, channels * SPAN, 2 * STEP, in_rows)
    gram = (2, inputs, inputs)
    operands = [
        pltpu.VMEM((depth, inputs), bf16),
        pltpu.VMEM((depth, inputs), bf16),
        pltpu.VMEM((inputs, depth), bf16),
    ]
    part, landed = pl.pallas_call(
        functools.partial(stream_kernel, n_inp, n_tm),
        out_shape=[pltpu.VMEM(gram, f32), pltpu.VMEM(tiles, bf16)],
        in_specs=[hbm, hbm, hbm],
        out_specs=[vmem, vmem],
        scratch_shapes=[
            pltpu.VMEM(pfb_coeff.shape, f32),
            pltpu.VMEM(table.shape, f32),
            pltpu.VMEM(voltages.shape, bf16),
            pltpu.VMEM((taps * lines, length), bf16),
            pltpu.VMEM((taps * lines, length), TINY),
            pltpu.VMEM((STEP // PART, PART * in_rows, length), TINY),
            pltpu.VMEM(carry, f32),
            pltpu.VMEM((heads, lines * STEP, in_rows), f32),
            pltpu.VMEM(carry, f32),
            pltpu.VMEM(carry, f32),
            pltpu.VMEM((lines * STEP, in_rows), f32),
            pltpu.VMEM((steps, channels, 2 * STEP, in_rows), bf16),
            *operands,
            pltpu.SemaphoreType.DMA((2,)),
            pltpu.SemaphoreType.DMA((steps,)),
            pltpu.SemaphoreType.DMA,
            pltpu.SemaphoreType.DMA,
            pltpu.SemaphoreType.DMA,
            pltpu.SemaphoreType.DMA((steps // SPAN,)),
        ],
        compiler_params=pltpu.CompilerParams(
            collective_id=0, has_side_effects=True, vmem_limit_bytes=44 * 1024 * 1024
        ),
        name="stream",
    )(*(pltpu.with_memory_space_constraint(x, pltpu.HBM) for x in (voltages, pfb_coeff, table)))
    return pl.pallas_call(
        functools.partial(close_kernel, n_tm * steps * STEP),
        out_shape=jax.ShapeDtypeStruct((1, *gram), f32),
        in_specs=[vmem, vmem],
        out_specs=hbm,
        scratch_shapes=[*operands, pltpu.VMEM(gram, f32), pltpu.SemaphoreType.DMA],
        compiler_params=pltpu.CompilerParams(vmem_limit_bytes=24 * 1024 * 1024),
        name="close",
    )(part, landed)


def per_device(voltages, pfb_coeff):
    if voltages.shape[0] % LANES == 0:
        return stream_device(voltages, pfb_coeff)
    return narrow_device(voltages, pfb_coeff)


def solution(mesh):
    return jax.shard_map(
        per_device,
        mesh=mesh,
        in_specs=(P("inp", "tm"), P()),
        out_specs=P(("inp", "tm"), None, None, None),
        check_vma=False,
    )
```

```python
import functools
import math

import jax
import jax.numpy as jnp
import numpy as np
from jax import lax
from jax.experimental import pallas as pl
from jax.experimental.pallas import tpu as pltpu
from jax.sharding import PartitionSpec as P

LANES = 128
ROWS = 16
GROUP = 8
CHUNK = 16
NT = (((1,), (1,)), ((), ()))


def dft_tables(channels, length):
    phase = np.arange(channels)[:, None] * np.arange(length)[None, :] % length
    angle = phase * (2.0 * math.pi / length)
    table = np.stack([np.cos(angle), -np.sin(angle)], axis=1) / math.sqrt(length)
    table = table.reshape(2 * channels, length).astype(np.float32)
    high = table.astype(jnp.bfloat16)
    low = (table - high.astype(np.float32)).astype(jnp.bfloat16)
    return np.concatenate([high, low], axis=0)


def channelize_kernel(
    n_inp, n_tm, volt, coef_in, table, out,
    slab, coef, high0, low0, high1, low1, stage, send,
    load_sem, tail_send, tail_recv, send_sem, recv_sem,
):
    in_rows = volt.shape[0]
    taps, length = coef_in.shape
    spec = volt.shape[1] // length
    lines = stage.shape[0] // CHUNK
    n_dev = n_inp * n_tm
    chunks = spec // CHUNK
    tail = (taps - 1) * length
    width = CHUNK * length
    a_tiles = in_rows // ROWS
    inp = lax.axis_index("inp")
    tm = lax.axis_index("tm")
    me = inp * n_tm + tm

    def load(q):
        return pltpu.make_async_copy(
            volt.at[:, pl.ds(pl.multiple_of(q * width, width), width)],
            slab.at[:, pl.ds(pl.multiple_of(tail + q * width, length), width)],
            load_sem.at[q],
        )

    load(0).start()
    load(1).start()

    barrier = pltpu.get_barrier_semaphore()

    def greet(d, _):
        other = lax.rem(me + d, n_dev)
        pl.semaphore_signal(
            barrier, inc=1, device_id=(other // n_tm, lax.rem(other, n_tm)),
            device_id_type=pl.DeviceIdType.MESH,
        )
        return _

    lax.fori_loop(1, n_dev, greet, 0)
    for j in range(taps):
        coef[j] = jnp.broadcast_to(coef_in[j : j + 1, :], (8, length))
    @pl.when(tm == 0)
    def _():
        def clear(e, _):
            slab[:, pl.ds(pl.multiple_of(e * length, length), length)] = jnp.zeros(
                (in_rows, length), slab.dtype
            )
            return _

        lax.fori_loop(0, taps - 1, clear, 0)

    f_high, f_low = (high0, high1), (low0, low1)

    def fir(first, tile, slot):
        row = pl.multiple_of(tile * ROWS, ROWS)
        for nt in range(length // LANES):
            lanes = pl.ds(nt * LANES, LANES)
            c = [coef[j, :, lanes] for j in range(taps)]
            low = [None] * GROUP
            high = [None] * GROUP
            for t in range(GROUP + taps - 1):
                col = pl.multiple_of((first + t) * length + nt * LANES, LANES)
                x = slab[pl.ds(row, ROWS), pl.ds(col, LANES)].astype(jnp.float32)
                x0, x1 = x[:8], x[8:]
                for i in range(max(0, t - taps + 1), min(GROUP - 1, t) + 1):
                    w = c[t - i]
                    if t == i:
                        low[i], high[i] = w * x0, w * x1
                    else:
                        low[i], high[i] = low[i] + w * x0, high[i] + w * x1
                i = t - taps + 1
                if i >= 0:
                    f = jnp.concatenate([low[i], high[i]], axis=0)
                    h = f.astype(jnp.bfloat16)
                    f_high[slot][i, pl.ds(row, ROWS), lanes] = h
                    f_low[slot][i, pl.ds(row, ROWS), lanes] = (
                        f - h.astype(jnp.float32)
                    ).astype(jnp.bfloat16)

    def dft(tile, slot):
        per = GROUP // a_tiles
        for u in range(per):
            i = tile * per + u
            r = lax.dot_general(table[...], f_high[slot][i], NT, preferred_element_type=jnp.float32)
            r2 = lax.dot_general(table[:lines], f_low[slot][i], NT, preferred_element_type=jnp.float32)
            stage[pl.ds(slot * GROUP + i, lines, stride=CHUNK), :] = r[:lines] + r[lines:] + r2

    def each(body):
        def step(tile, _):
            body(tile)
            return _

        lax.fori_loop(0, a_tiles, step, 0)

    def own(q):
        return pltpu.make_async_copy(send.at[q, me], place(out, q), recv_sem)

    def place(ref, q):
        first = pl.multiple_of(tm * spec + q * CHUNK, CHUNK)
        return ref.at[inp, :, pl.ds(first, CHUNK), :]

    def dispatch(q):
        def convert(d, _):
            rows = pl.ds(pl.multiple_of(d * 2 * CHUNK, 2 * CHUNK), 2 * CHUNK)
            send[q, d] = stage[rows, :].reshape(2, CHUNK, in_rows).astype(send.dtype)
            return _

        lax.fori_loop(0, n_dev, convert, 0)

        def post(d, _):
            other = lax.rem(me + d, n_dev)
            pltpu.make_async_remote_copy(
                src_ref=send.at[q, other], dst_ref=place(out, q),
                send_sem=send_sem, recv_sem=recv_sem,
                device_id=(other // n_tm, lax.rem(other, n_tm)),
                device_id_type=pl.DeviceIdType.MESH,
            ).start()
            return _

        lax.fori_loop(1, n_dev, post, 0)
        own(q).start()

    def chunk_of(k):
        return lax.rem(k + 1, chunks)

    load(0).wait()
    load(1).wait()
    for q in range(2, chunks):
        load(q).start()
    each(lambda tile: fir(chunk_of(0) * CHUNK, tile, 0))
    pl.semaphore_wait(barrier, n_dev - 1)

    history = pltpu.make_async_remote_copy(
        src_ref=volt.at[:, pl.ds(spec * length - tail, tail)],
        dst_ref=slab.at[:, pl.ds(0, tail)],
        send_sem=tail_send, recv_sem=tail_recv,
        device_id=(inp, lax.rem(tm + 1, n_tm)),
        device_id_type=pl.DeviceIdType.MESH,
    )

    @pl.when(tm < n_tm - 1)
    def _():
        history.start()

    def turn(k, carry):
        q = chunk_of(k)
        later = chunk_of(k + 1)

        def second(tile):
            dft(tile, 0)
            fir(q * CHUNK + GROUP, tile, 1)

        each(second)

        @pl.when(later > 0)
        def _():
            load(later).wait()

        @pl.when((later == 0) & (tm > 0))
        def _():
            history.wait_recv()

        def first(tile):
            dft(tile, 1)
            fir(later * CHUNK, tile, 0)

        each(first)
        dispatch(q)
        return carry

    lax.fori_loop(0, chunks - 1, turn, 0)

    def final(tile):
        dft(tile, 0)
        fir(GROUP, tile, 1)

    each(final)
    each(lambda tile: dft(tile, 1))
    dispatch(0)

    @pl.when(tm < n_tm - 1)
    def _():
        history.wait_send()

    sent = send.at[:, pl.ds(0, n_dev - 1)]
    pltpu.make_async_copy(sent, sent, send_sem).wait()
    pltpu.make_async_copy(out, out, recv_sem).wait()


def correlate_kernel(z_ref, o_ref, wide, turned, crossed):
    groups, _, spectra, in_rows = z_ref.shape
    block = o_ref.shape[2]

    @pl.when(pl.program_id(0) == 0)
    def _():
        for g in range(groups):
            cols = slice(g * in_rows, (g + 1) * in_rows)
            for p in range(2):
                part = z_ref[g, p]
                wide[p * spectra : (p + 1) * spectra, cols] = part
                flip = part.T
                turned[cols, p * spectra : (p + 1) * spectra] = flip
                crossed[cols, (1 - p) * spectra : (2 - p) * spectra] = flip if p else -flip

    rows = pl.ds(pl.multiple_of(pl.program_id(0) * block, block), block)
    scale = 1.0 / spectra
    o_ref[0, 0] = jnp.dot(turned[rows, :], wide[...], preferred_element_type=jnp.float32) * scale
    o_ref[0, 1] = jnp.dot(crossed[rows, :], wide[...], preferred_element_type=jnp.float32) * scale


def narrow_device(voltages, pfb_coeff):
    n_inp = lax.axis_size("inp")
    n_tm = lax.axis_size("tm")
    channels = n_inp * n_tm
    in_rows = voltages.shape[0]
    taps, length = pfb_coeff.shape
    spec = voltages.shape[1] // length
    lines = 2 * channels
    table = jnp.asarray(dft_tables(channels, length))
    vmem = pl.BlockSpec(memory_space=pltpu.VMEM)
    hbm = pl.BlockSpec(memory_space=pl.ANY)
    bf16 = jnp.bfloat16
    received = pl.pallas_call(
        functools.partial(channelize_kernel, n_inp, n_tm),
        out_shape=jax.ShapeDtypeStruct((n_inp, 2, n_tm * spec, in_rows), bf16),
        in_specs=[hbm, vmem, vmem],
        out_specs=hbm,
        scratch_shapes=[
            pltpu.VMEM((in_rows, (spec + taps - 1) * length), bf16),
            pltpu.VMEM((taps, 8, length), jnp.float32),
            pltpu.VMEM((GROUP, in_rows, length), bf16),
            pltpu.VMEM((GROUP, in_rows, length), bf16),
            pltpu.VMEM((GROUP, in_rows, length), bf16),
            pltpu.VMEM((GROUP, in_rows, length), bf16),
            pltpu.VMEM((lines * CHUNK, in_rows), jnp.float32),
            pltpu.VMEM((spec // CHUNK, channels, 2, CHUNK, in_rows), bf16),
            pltpu.SemaphoreType.DMA((spec // CHUNK,)),
            pltpu.SemaphoreType.DMA,
            pltpu.SemaphoreType.DMA,
            pltpu.SemaphoreType.DMA,
            pltpu.SemaphoreType.DMA,
        ],
        compiler_params=pltpu.CompilerParams(
            collective_id=0, has_side_effects=True, vmem_limit_bytes=60 * 1024 * 1024
        ),
        name="channelize",
    )(voltages, pfb_coeff, table)
    inputs = n_inp * in_rows
    spectra = n_tm * spec
    block = min(256, inputs)
    return pl.pallas_call(
        correlate_kernel,
        grid=(inputs // block,),
        out_shape=jax.ShapeDtypeStruct((1, 2, inputs, inputs), jnp.float32),
        in_specs=[pl.BlockSpec(received.shape, lambda i: (0, 0, 0, 0))],
        out_specs=pl.BlockSpec((1, 2, block, inputs), lambda i: (0, 0, i, 0)),
        scratch_shapes=[
            pltpu.VMEM((2 * spectra, inputs), bf16),
            pltpu.VMEM((inputs, 2 * spectra), bf16),
            pltpu.VMEM((inputs, 2 * spectra), bf16),
        ],
        compiler_params=pltpu.CompilerParams(vmem_limit_bytes=60 * 1024 * 1024),
        name="correlate",
    )(received)


STEP = 8
PART = 4
SPAN = 4
BLOCK = 256
AHEAD = 3
TINY = jnp.float8_e5m2
LIFT = 2.0**12
GAIN = 2.0**38


def split_table(channels, length):
    phase = np.arange(channels)[:, None] * np.arange(length)[None, :] % length
    angle = phase * (2.0 * math.pi / length)
    table = np.stack([np.cos(angle), -np.sin(angle)], axis=1) / math.sqrt(length)
    return table.reshape(2 * channels, length).astype(np.float32)


def stream_kernel(
    n_inp, n_tm, volt, coef_from, table_from, part, landed,
    coef_in, table, slab, taps_table, low_table, thin, acc, head, tail_out, tail_in, stage, send,
    wide, cross, turned, small_sem, load_sem, tail_send, tail_recv, send_sem, recv_sem,
):
    in_rows = volt.shape[0]
    taps, length = coef_from.shape
    steps = volt.shape[1] // (length * STEP)
    lines = table_from.shape[0]
    n_dev = n_inp * n_tm
    width = STEP * length
    inp = lax.axis_index("inp")
    tm = lax.axis_index("tm")
    me = inp * n_tm + tm
    heads = (taps + STEP - 1) // STEP
    origin = steps // 2
    turn = steps - origin

    def load(i):
        cols = pl.ds(pl.multiple_of(i * width, width), width)
        return pltpu.make_async_copy(volt.at[:, cols], slab.at[:, cols], load_sem.at[i])

    small = [
        pltpu.make_async_copy(source, target, small_sem.at[n])
        for n, (source, target) in enumerate(((coef_from, coef_in), (table_from, table)))
    ]
    for copy in small:
        copy.start()
    for t in range(AHEAD):
        load((t + origin) % steps).start()

    barrier = pltpu.get_barrier_semaphore()

    def greet(d, _):
        other = lax.rem(me + d, n_dev)
        pl.semaphore_signal(
            barrier, inc=1, device_id=(other // n_tm, lax.rem(other, n_tm)),
            device_id_type=pl.DeviceIdType.MESH,
        )
        return _

    lax.fori_loop(1, n_dev, greet, 0)
    acc[...] = jnp.zeros(acc.shape, acc.dtype)
    for copy in small:
        copy.wait()

    early = min(STEP + taps - 1 - heads * STEP, taps)

    def build(j, _):
        full = table[...] * coef_in[pl.ds(j, 1), :] * GAIN
        high = full.astype(jnp.bfloat16)
        rows = pl.ds(j * lines if isinstance(j, int) else pl.multiple_of(j * lines, lines), lines)
        taps_table[rows, :] = high
        low_table[rows, :] = ((full - high.astype(jnp.float32)) / LIFT).astype(TINY)
        return _

    lax.fori_loop(0, early, build, 0)

    half = n_inp // 2
    side = inp // half
    fars = [(1 - side) * half + lax.rem(inp + d, half) for d in range(half)]
    nears = [side * half + lax.rem(inp + d, half) for d in range(half)]
    cores = [lax.rem(tm + d, n_tm) for d in range(n_tm)]

    def dispatch(i, place, far_first=True):
        send[i] = (stage[...] * (1.0 / GAIN)).reshape(n_dev, 2 * STEP, in_rows).astype(send.dtype)
        group = place // SPAN
        target = landed.at[group, me * SPAN + place % SPAN]

        def post(inp2, tm2):
            pltpu.make_async_remote_copy(
                src_ref=send.at[i, inp2 * n_tm + tm2], dst_ref=target,
                send_sem=send_sem, recv_sem=recv_sem.at[group],
                device_id=(inp2, tm2), device_id_type=pl.DeviceIdType.MESH,
            ).start()

        far = [(row, core) for row in fars for core in cores]
        near = [(row, core) for row in nears for core in cores][1:]
        for row, core in far + near if far_first else near + far:
            post(row, core)
        target[...] = send[i, me]

    def advance(i, skip=0, stop=STEP + taps - 1):
        first = i * width
        for h in range(STEP // PART):
            start = max(skip - h * PART, 0)
            end = min(stop - h * PART, PART + taps - 1)
            base = max(taps - end, 0) * lines
            used = min(PART + taps - 1 - start, taps) * lines
            x = jnp.concatenate(
                [
                    slab[:, pl.ds(pl.multiple_of(first + (h * PART + u) * length, length), length)]
                    for u in range(PART)
                ],
                axis=0,
            )
            thin[h] = (x.astype(jnp.float32) * LIFT).astype(TINY)
            high = lax.dot_general(taps_table[base:used, :], x, NT, preferred_element_type=jnp.float32)
            low = lax.dot_general(low_table[base:used, :], thin[h], NT, preferred_element_type=jnp.float32)
            for k in range(start, end):
                total = acc[k] if k < taps - 1 else None
                for u in range(PART):
                    j = u + taps - 1 - k
                    if 0 <= j < taps:
                        spot = (slice(j * lines - base, (j + 1) * lines - base), slice(u * in_rows, (u + 1) * in_rows))
                        term = high[spot] + low[spot]
                        total = term if total is None else total + term
                if k < PART:
                    stage[pl.ds(h * PART + k, lines, stride=STEP), :] = total
                else:
                    acc[k - PART] = total

    def finish(q):
        for k in range(STEP):
            rows = pl.ds(k, lines, stride=STEP)
            total = head[q, rows, :]
            s = q * STEP + k
            stage[rows, :] = total + tail_in[s] if s < taps - 1 else total
        dispatch(q, steps - heads + q, False)

    history = pltpu.make_async_remote_copy(
        src_ref=tail_out, dst_ref=tail_in, send_sem=tail_send, recv_sem=tail_recv,
        device_id=(inp, lax.rem(tm + 1, n_tm)), device_id_type=pl.DeviceIdType.MESH,
    )

    for t in range(heads):
        load(t + origin).wait()
        load((t + origin + AHEAD) % steps).start()
        advance(t + origin, (heads - t) * STEP)
        if t == 0:
            for j in range(early, taps):
                build(j, None)
    load(origin + heads).wait()
    load((origin + heads + AHEAD) % steps).start()
    pl.semaphore_wait(barrier, n_dev - 1)
    advance(origin + heads, 0, STEP)
    dispatch(origin + heads, 0)
    advance(origin + heads, STEP)

    def work(t, carry):
        i = lax.rem(t + origin, steps)

        @pl.when(t < steps)
        def _():
            load(i).wait()

        @pl.when(t < steps - AHEAD)
        def _():
            load(lax.rem(i + AHEAD, steps)).start()

        @pl.when(t == turn)
        def _():
            tail_out[...] = acc[...]
            acc[...] = jnp.zeros(acc.shape, acc.dtype)

            @pl.when(tm < n_tm - 1)
            def _():
                history.start()

        advance(i)

        @pl.when(i < heads)
        def _():
            head[i] = stage[...]

        @pl.when(i >= heads)
        def _():
            dispatch(i, lax.rem(i + steps - 2 * heads - origin, steps - heads))

        return carry

    lax.fori_loop(heads + 1, steps + heads, work, 0)

    @pl.when(tm > 0)
    def _():
        history.wait_recv()

    @pl.when(tm == 0)
    def _():
        tail_in[...] = jnp.zeros(tail_in.shape, tail_in.dtype)

    for q in range(heads):
        finish(q)

    def arrive(group):
        came = landed.at[group, pl.ds(0, (n_dev - 1) * SPAN)]
        pltpu.make_async_copy(came, came, recv_sem.at[group]).wait()

    def fold(group):
        arrive(group)
        pack(landed.at[group], wide, cross, turned)

        def block(b, carry):
            rows = pl.ds(pl.multiple_of(b * BLOCK, BLOCK), BLOCK)
            left = turned[rows, :]
            for p, right in enumerate((wide, cross)):
                term = jnp.dot(left, right[...], preferred_element_type=jnp.float32)
                part[p, rows, :] = term if group == 0 else part[p, rows, :] + term
            return carry

        lax.fori_loop(0, part.shape[1] // BLOCK, block, 0)

    for group in range(steps // SPAN - 1):
        fold(group)

    @pl.when(tm < n_tm - 1)
    def _():
        history.wait_send()

    sent = send.at[:, pl.ds(0, n_dev - 1)]
    pltpu.make_async_copy(sent, sent, send_sem).wait()
    arrive(steps // SPAN - 1)


def pack(source, wide, cross, turned):
    depth, inputs = wide.shape
    tiles, pair, in_rows = source.shape
    span = depth // pair
    for g in range(inputs // in_rows):
        cols = slice(g * in_rows, (g + 1) * in_rows)
        piece = source[g * span : (g + 1) * span]
        flat = piece.reshape(depth, in_rows)
        wide[:, cols] = flat
        turned[cols, :] = flat.T
        full = piece.astype(jnp.float32)
        swap = jnp.concatenate([-full[:, pair // 2 :], full[:, : pair // 2]], axis=1)
        cross[:, cols] = swap.astype(piece.dtype).reshape(depth, in_rows)


def close_kernel(spectra, part, landed, out, wide, cross, turned, done, sem):
    pack(landed.at[landed.shape[0] - 1], wide, cross, turned)
    scale = 1.0 / spectra
    copies = []
    edges = [0, BLOCK // 2, *range(BLOCK, part.shape[1] + 1, BLOCK)]
    for low, high in zip(edges, edges[1:]):
        rows = slice(low, high)
        left = turned[rows, :]
        for p, right in enumerate((wide, cross)):
            term = jnp.dot(left, right[...], preferred_element_type=jnp.float32)
            done[p, rows, :] = (part[p, rows, :] + term) * scale
            copies.append(
                pltpu.make_async_copy(done.at[p, rows, :], out.at[0, p, rows, :], sem)
            )
            copies[-1].start()
    pltpu.make_async_copy(done, out.at[0], sem).wait()


def stream_device(voltages, pfb_coeff):
    n_inp = lax.axis_size("inp")
    n_tm = lax.axis_size("tm")
    channels = n_inp * n_tm
    in_rows = voltages.shape[0]
    taps, length = pfb_coeff.shape
    steps = voltages.shape[1] // (length * STEP)
    lines = 2 * channels
    heads = (taps + STEP - 1) // STEP
    table = jnp.asarray(split_table(channels, length))
    vmem = pl.BlockSpec(memory_space=pltpu.VMEM)
    hbm = pl.BlockSpec(memory_space=pl.ANY)
    bf16, f32 = jnp.bfloat16, jnp.float32
    carry = (taps - 1, lines, in_rows)
    inputs = n_inp * in_rows
    depth = n_tm * SPAN * 2 * STEP
    tiles = (steps // SPAN, channels * SPAN, 2 * STEP, in_rows)
    gram = (2, inputs, inputs)
    operands = [
        pltpu.VMEM((depth, inputs), bf16),
        pltpu.VMEM((depth, inputs), bf16),
        pltpu.VMEM((inputs, depth), bf16),
    ]
    part, landed = pl.pallas_call(
        functools.partial(stream_kernel, n_inp, n_tm),
        out_shape=[pltpu.VMEM(gram, f32), pltpu.VMEM(tiles, bf16)],
        in_specs=[hbm, hbm, hbm],
        out_specs=[vmem, vmem],
        scratch_shapes=[
            pltpu.VMEM(pfb_coeff.shape, f32),
            pltpu.VMEM(table.shape, f32),
            pltpu.VMEM(voltages.shape, bf16),
            pltpu.VMEM((taps * lines, length), bf16),
            pltpu.VMEM((taps * lines, length), TINY),
            pltpu.VMEM((STEP // PART, PART * in_rows, length), TINY),
            pltpu.VMEM(carry, f32),
            pltpu.VMEM((heads, lines * STEP, in_rows), f32),
            pltpu.VMEM(carry, f32),
            pltpu.VMEM(carry, f32),
            pltpu.VMEM((lines * STEP, in_rows), f32),
            pltpu.VMEM((steps, channels, 2 * STEP, in_rows), bf16),
            *operands,
            pltpu.SemaphoreType.DMA((2,)),
            pltpu.SemaphoreType.DMA((steps,)),
            pltpu.SemaphoreType.DMA,
            pltpu.SemaphoreType.DMA,
            pltpu.SemaphoreType.DMA,
            pltpu.SemaphoreType.DMA((steps // SPAN,)),
        ],
        compiler_params=pltpu.CompilerParams(
            collective_id=0, has_side_effects=True, vmem_limit_bytes=44 * 1024 * 1024
        ),
        name="stream",
    )(*(pltpu.with_memory_space_constraint(x, pltpu.HBM) for x in (voltages, pfb_coeff, table)))
    return pl.pallas_call(
        functools.partial(close_kernel, n_tm * steps * STEP),
        out_shape=jax.ShapeDtypeStruct((1, *gram), f32),
        in_specs=[vmem, vmem],
        out_specs=hbm,
        scratch_shapes=[*operands, pltpu.VMEM(gram, f32), pltpu.SemaphoreType.DMA],
        compiler_params=pltpu.CompilerParams(vmem_limit_bytes=24 * 1024 * 1024),
        name="close",
    )(part, landed)


def per_device(voltages, pfb_coeff):
    if voltages.shape[0] % LANES == 0:
        return stream_device(voltages, pfb_coeff)
    return narrow_device(voltages, pfb_coeff)


def solution(mesh):
    return jax.shard_map(
        per_device,
        mesh=mesh,
        in_specs=(P("inp", "tm"), P()),
        out_specs=P(("inp", "tm"), None, None, None),
        check_vma=False,
    )
```
